32 devices in a mesh: row: 4 (over y, core), col: 4 (over z), dp: 2 (over x).
Axes of the slice: x: 2, y: 2, z: 4, core: 2. Of those that a mesh axis runs over, the one named last changes fastest.
Arguments:
- observed: bfloat16 [1024, 2048], P(('row', 'dp'), 'col'), may hold values from -6 to 6
- next_observed: bfloat16 [1024, 2048], P(('row', 'dp'), 'col'), may hold values from -6 to 6
- actions: bfloat16 [1024, 128], P(('row', 'dp')), may hold values from -1 to 1
- next_mean: bfloat16 [1024, 128], P(('row', 'dp')), may hold values from -1.1953125 to 1.1953125
- policy_noise: float32 [1024, 128], P(('row', 'dp')), may hold values from -1.5 to 1.5
- rewards: bfloat16 [1024], P(('row', 'dp')), may hold values from -5 to 5
- discounts: bfloat16 [1024], P(('row', 'dp')), may hold values from 0.5 to 0.98828125
- actor_flags: int32 [1024], P(('row', 'dp')), may hold values 0 or 1
- critic_in: float32 [2, 2048, 2048], P(None, 'col', 'row'), may hold values from -0.125 to 0.125
- critic_act: float32 [2, 128, 2048], P(None, None, 'col'), may hold values from -0.5 to 0.5
- critic_head: float32 [2, 2048], P(None, 'row'), may hold values from -0.125 to 0.125
- target_in: float32 [2, 2048, 2048], P(None, 'col', 'row'), may hold values from -0.125 to 0.125
- target_act: float32 [2, 128, 2048], P(None, None, 'col'), may hold values from -0.5 to 0.5
- target_head: float32 [2, 2048], P(None, 'row'), may hold values from -0.125 to 0.125
Outputs:
- new_in: float32 [2, 2048, 2048], P(None, 'col', 'row')
- new_act: float32 [2, 128, 2048], P(None, None, 'col')
- new_head: float32 [2, 2048], P(None, 'row')
- new_target_in: float32 [2, 2048, 2048], P(None, 'col', 'row')
- new_target_act: float32 [2, 128, 2048], P(None, None, 'col')
- new_target_head: float32 [2, 2048], P(None, 'row')
- temporal_errors: float32 [2, 1024], P(None, ('row', 'dp'))
- action_slope: float32 [1024, 128], P(('row', 'dp'))
The draws below stay inside these ranges and needn't reach their ends.
All inputs are finite; a program needn't handle non-finite values. No bound on the sum of `actor_flags` on one device may be relied on, other than what follows from the above.
Results may differ from the reference program's by a relative error of at most 0.008.
Values may be sent and summed in bfloat16 or wider, within the bound.
A program may use at most 128 MiB of HBM per device.

```python
import jax
import jax.numpy as jnp
from jax import lax

D = 2048
ACT = 128
TOKENS = 1024


def place_ends(drawn, rng, smallest, high):
    shape = drawn.shape
    index_at = [jax.random.randint(jax.random.fold_in(rng, axis), (), 0, shape[axis]) for axis in range(len(shape))]
    drawn = drawn.at[tuple(index_at)].set(smallest)
    longest = shape.index(max(shape))
    index_at[longest] = (index_at[longest] + 1) % shape[longest]
    return drawn.at[tuple(index_at)].set(high)


def level_of(key, dims, split, low, high):
    def one(dim, parts):
        draws = jax.random.uniform(jax.random.fold_in(jax.random.fold_in(key, 6), dim), (parts,), jnp.float32, low / len(split), high / len(split))
        return jnp.repeat(jnp.exp(draws), dims[dim] // parts).reshape((-1,) + (1,) * (len(dims) - dim - 1))

    factor_of = one(*split[0])
    for cut in split[1:]:
        factor_of = factor_of * one(*cut)
    return factor_of


def gaussian(own_key, shape, width, reach, pieces=(), held_as=jnp.bfloat16):
    values = jax.random.normal(own_key, shape, jnp.float32) * width
    if len(pieces) > 0:
        values = level_of(own_key, shape, pieces, -0.22, 0.18) * values
    return jnp.clip(values, min=-reach, max=reach).astype(held_as)


def setup_inputs(seed: int = 0) -> dict:
    seeds = jax.random.split(jax.random.key(seed), 15)
    return {
        "observed": gaussian(seeds[0], (TOKENS, D), 1.0, 6.0, ((0, 8), (1, 4))),
        "next_observed": gaussian(seeds[1], (TOKENS, D), 1.0, 6.0, ((0, 8), (1, 4))),
        "actions": jnp.clip(jax.random.uniform(seeds[2], (TOKENS, ACT), jnp.float32, -1.0, 1.0) * level_of(seeds[2], (TOKENS, ACT), ((0, 8),), -0.4, 0.0), -1.0, 1.0).astype(jnp.bfloat16),
        "next_mean": jnp.clip(jax.random.uniform(seeds[3], (TOKENS, ACT), jnp.float32, -1.1953125, 1.1953125) * level_of(seeds[3], (TOKENS, ACT), ((0, 8),), -0.4, 0.0), -1.1953125, 1.1953125).astype(jnp.bfloat16),
        "policy_noise": gaussian(seeds[4], (TOKENS, ACT), 0.3, 1.5, ((0, 8),), jnp.float32),
        "rewards": gaussian(seeds[5], (TOKENS,), 1.0, 5.0, ((0, 8),)),
        "discounts": jnp.clip(0.5 + 0.48828125 * jax.random.uniform(seeds[6], (TOKENS,), jnp.float32) ** level_of(seeds[6], (TOKENS,), ((0, 8),), -0.2, 0.2), 0.5, 0.98828125).astype(jnp.bfloat16),
        "actor_flags": place_ends((jax.random.randint(seeds[7], (TOKENS,), 0, 2) < 1).astype(jnp.int32), jax.random.fold_in(seeds[7], 1), 0, 1),
        "critic_in": gaussian(seeds[8], (2, D, D), D ** -0.5, 0.125, ((1, 4), (2, 4)), jnp.float32),
        "critic_act": gaussian(seeds[9], (2, ACT, D), ACT ** -0.5, 0.5, ((2, 4),), jnp.float32),
        "critic_head": gaussian(seeds[10], (2, D), D ** -0.5, 0.125, ((1, 4),), jnp.float32),
        "target_in": gaussian(seeds[11], (2, D, D), D ** -0.5, 0.125, ((1, 4), (2, 4)), jnp.float32),
        "target_act": gaussian(seeds[12], (2, ACT, D), ACT ** -0.5, 0.5, ((2, 4),), jnp.float32),
        "target_head": gaussian(seeds[13], (2, D), D ** -0.5, 0.125, ((1, 4),), jnp.float32),
    }


noise_clip = 0.5
matrix_rate = 0.004
head_rate = 0.0001
blend_rate = 0.005


def silu_slope(preact):
    sigma = jax.nn.sigmoid(preact)
    return sigma * (1.0 + preact * (1.0 - sigma))


def forward(states, moves, weight_in, weight_act, weight_head):
    embedded = (states.astype(jnp.float32) + jnp.dot(moves, weight_act.astype(jnp.bfloat16), preferred_element_type=jnp.float32)).astype(jnp.bfloat16)
    preact = jnp.dot(embedded, weight_in.astype(jnp.bfloat16), preferred_element_type=jnp.float32)
    hidden = jax.nn.silu(preact)
    value = jnp.dot(hidden, weight_head, precision=lax.Precision.HIGHEST)
    return embedded, preact, hidden, value


def reference(observed, next_observed, actions, next_mean, policy_noise, rewards, discounts, actor_flags, critic_in, critic_act, critic_head, target_in, target_act, target_head):
    noisy = jnp.clip(next_mean.astype(jnp.float32) + jnp.clip(policy_noise, -noise_clip, noise_clip), -1.0, 1.0).astype(jnp.bfloat16)
    target_zero = forward(next_observed, noisy, target_in[0], target_act[0], target_head[0])[3]
    target_one = forward(next_observed, noisy, target_in[1], target_act[1], target_head[1])[3]
    goal = rewards.astype(jnp.float32) + discounts.astype(jnp.float32) * jnp.minimum(target_zero, target_one)
    fresh_in = []
    fresh_act = []
    fresh_head = []
    errors = []
    action_slope = None
    for which in range(2):
        embedded, preact, hidden, value = forward(observed, actions, critic_in[which], critic_act[which], critic_head[which])
        error = value - goal
        slope = (critic_head[which] * silu_slope(preact)).astype(jnp.bfloat16)
        delta = (2.0 * error[:, None] * slope.astype(jnp.float32)).astype(jnp.bfloat16)
        back = jnp.dot(slope, critic_in[which].astype(jnp.bfloat16).T, preferred_element_type=jnp.float32)
        grad_embedded = (2.0 * error[:, None] * back).astype(jnp.bfloat16)
        grad_in = jnp.dot(embedded.T, delta, preferred_element_type=jnp.float32)
        grad_act = jnp.dot(actions.T, grad_embedded, preferred_element_type=jnp.float32)
        grad_head = jnp.dot(2.0 * error, hidden, precision=lax.Precision.HIGHEST)
        fresh_in.append(critic_in[which] - matrix_rate * grad_in)
        fresh_act.append(critic_act[which] - matrix_rate * grad_act)
        fresh_head.append(critic_head[which] - head_rate * grad_head)
        errors.append(error)
        if which == 0:
            push = jnp.dot(back.astype(jnp.bfloat16), critic_act[0].astype(jnp.bfloat16).T, preferred_element_type=jnp.float32)
            action_slope = actor_flags.astype(jnp.float32)[:, None] * push
    new_in = jnp.stack(fresh_in)
    new_act = jnp.stack(fresh_act)
    new_head = jnp.stack(fresh_head)
    new_target_in = blend_rate * new_in + (1.0 - blend_rate) * target_in
    new_target_act = blend_rate * new_act + (1.0 - blend_rate) * target_act
    new_target_head = blend_rate * new_head + (1.0 - blend_rate) * target_head
    return new_in, new_act, new_head, new_target_in, new_target_act, new_target_head, jnp.stack(errors), action_slope
```

```python
import functools

import jax
import jax.numpy as jnp
from jax import lax
from jax.experimental import pallas as pl
from jax.experimental.pallas import tpu as pltpu
from jax.sharding import PartitionSpec as P

noise_clip = 0.5
matrix_rate = 0.004
head_rate = 0.0001
blend_rate = 0.005

f32 = jnp.float32
bf16 = jnp.bfloat16
skew = 2


def kernel(dims, observed_at, next_observed_at, actions_at, next_mean_at, noise_at, rewards_at,
           discounts_at, flags_at, cin_at, cact_at, chead_at, tin_at, tact_at, thead_at, new_in, new_act, new_head, new_tin, new_tact,
           new_thead, errs_out, push_out, on_own, tg_own, heads, flag_column, columns,
           w16, a16, on_all, tg_all, emb, slopes, delta, rs_out, rs_in, hidden, vals, vt_own, vt_in,
           errs, gh, epad, ga_own, ga_out, ga_in, ga_all, pu_out, pu_in, pz_all,
           on_s, on_r, tg_s, tg_r, fon_s, fon_r, ftg_s, ftg_r, xon_s, xon_r,
           rs_s, rs_r, sl_s, sl_r, xs_s, xs_r, vt_s, vt_r, er_s, er_r, gh_s, gh_r,
           ga_s, ga_r, gb_s, gb_r, pu_s, pu_r, pz_s, pz_r, next_mean, noise, rewards, discounts,
           flags, cin, cact, chead, tin, tact, thead, load_s):
    R, C, D, TB, F, H, A = dims
    HI = R // 2
    TC = TB // 2
    row, col, dp = lax.axis_index("row"), lax.axis_index("col"), lax.axis_index("dp")
    hi, lo = row // 2, row % 2
    n = 8 * HI
    m = n // 2

    def copy(src, dst, ssem, rsem, **where):
        return pltpu.make_async_remote_copy(
            src_ref=src, dst_ref=dst, send_sem=ssem, recv_sem=rsem,
            device_id=where, device_id_type=pl.DeviceIdType.MESH)

    pairs = [(observed_at, on_own.at[:, :F]), (actions_at, on_own.at[:, F:]),
             (next_observed_at, tg_own.at[:, :F]), (next_mean_at, next_mean), (noise_at, noise),
             (rewards_at, rewards), (discounts_at, discounts), (flags_at, flags),
             (cact_at, cact), (cin_at.at[0], cin.at[0]), (cin_at.at[1], cin.at[1]),
             (tact_at, tact), (tin_at.at[0], tin.at[0]), (tin_at.at[1], tin.at[1]),
             (chead_at, chead), (thead_at, thead)]
    loads = [pltpu.make_async_copy(src, dst, load_s.at[x]) for x, (src, dst) in enumerate(pairs)]
    for load in loads:
        load.start()

    plane = [(c, d) for d in range(D) for c in range(C) if c or d]
    barrier = pltpu.get_barrier_semaphore()
    for o in range(1, R):
        pl.semaphore_signal(barrier, inc=1, device_id={"row": (row + o) % R},
                            device_id_type=pl.DeviceIdType.MESH)
    for c, d in plane:
        pl.semaphore_signal(barrier, inc=1,
                            device_id={"col": (col + c) % C, "dp": (dp + d) % D},
                            device_id_type=pl.DeviceIdType.MESH)
    pl.semaphore_wait(barrier, R - 1 + len(plane))

    def on_copy(o):
        to = hi * 2 + (1 - lo) if o == 0 else ((hi + o) % HI) * 2 + lo
        return copy(on_own, on_all.at[dp, row], on_s.at[o], on_r.at[o], row=to)

    def tg_copy(o):
        to = hi * 2 + (1 - lo) if o == 0 else ((hi + o) % HI) * 2 + lo
        return copy(tg_own, tg_all.at[row], tg_s.at[o], tg_r.at[o], row=to)

    for x in range(2):
        loads[x].wait()
    for o in range(HI):
        on_copy(o).start()
    for x in range(2, 8):
        loads[x].wait()
    tg_own[:, F:F + A] = jnp.clip(
        next_mean[...].astype(f32) + jnp.clip(noise[...], -noise_clip, noise_clip), -1.0, 1.0
    ).astype(bf16)
    epad[...] = jnp.zeros_like(epad)
    epad[4:5, :] = rewards[...].astype(f32)
    epad[5:6, :] = discounts[...].astype(f32)
    tg_own[:, F + A:] = epad[...].T.astype(bf16)
    epad[0:1, :] = flags[...].astype(f32)
    flag_column[...] = epad[...].T[:, 0:1]
    for o in range(HI):
        tg_copy(o).start()
    on_all[dp, row] = on_own[...]
    tg_all[row] = tg_own[...]
    for x in range(8, 16):
        loads[x].wait()
    for k in range(2):
        heads[k] = chead[k:k + 1, :]
        heads[2 + k] = thead[k:k + 1, :]
    for k in range(2):
        w16[k] = cin[k].astype(bf16)
        w16[2 + k] = tin[k].astype(bf16)
        a16[k] = cact[k].astype(bf16)
        a16[2 + k] = tact[k].astype(bf16)

    def fon_copy(o, block):
        return copy(on_all.at[dp, block], on_all.at[dp, block], fon_s.at[o], fon_r.at[o],
                    row=hi * 2 + (1 - lo))

    def ftg_copy(o, block):
        return copy(tg_all.at[block], tg_all.at[block], ftg_s.at[o], ftg_r.at[o],
                    row=hi * 2 + (1 - lo))

    def xon_copy(a, o, block, e):
        return copy(on_all.at[dp, block], on_all.at[dp, block], xon_s.at[a, o, e - 1],
                    xon_r.at[a, o, e - 1], dp=(dp + e) % D)

    def rows_of(d, block):
        return pl.ds(pl.multiple_of((d * R + block) * TB, TB), TB)

    def embed_on(d, block):
        x = on_all[d, block]
        for k in range(2):
            mixed = jnp.dot(x[:, F:], a16[k], preferred_element_type=f32)
            emb[k, rows_of(d, block), :] = (x[:, :F].astype(f32) + mixed).astype(bf16)

    def embed_tg(block):
        x = tg_all[block]
        for k in range(2):
            mixed = jnp.dot(x[:, F:F + A], a16[2 + k], preferred_element_type=f32)
            emb[k, rows_of(D, block), :] = (x[:, :F].astype(f32) + mixed).astype(bf16)

    def prepare(a, i):
        block_of = lambda o: ((hi + o) % HI) * 2 + a
        for o in range(HI):
            block = block_of(o)

            @pl.when(i == 4 * o)
            def _():
                @pl.when(lo == a)
                def _():
                    if o > 0:
                        on_copy(o).wait_recv()
                        fon_copy(o, block).start()

                @pl.when(lo != a)
                def _():
                    if o > 0:
                        fon_copy(o, block).wait_recv()
                    else:
                        on_copy(0).wait_recv()
                for e in range(1, D):
                    xon_copy(a, o, block, e).start()
                embed_on(dp, block)

            @pl.when(i == 4 * (HI + o))
            def _():
                @pl.when(lo == a)
                def _():
                    if o > 0:
                        tg_copy(o).wait_recv()
                        ftg_copy(o, block).start()

                @pl.when(lo != a)
                def _():
                    if o > 0:
                        ftg_copy(o, block).wait_recv()
                    else:
                        tg_copy(0).wait_recv()
                embed_tg(block)

    def place(a, i):
        group = i // (4 * HI)
        o = (i // 4) % HI
        kk = (i // 2) % 2
        half = i % 2
        there = (hi + o) % HI
        return group, kk, half, there, there * 2 + a

    def rs_copy(a, i):
        to = (col + 1) % C if a == 0 else (col + C - 1) % C
        return copy(rs_out.at[a, i], rs_in.at[a, i], rs_s.at[a, i], rs_r.at[a, i], col=to)

    def slope_at(d, kk, block, half):
        start = (d * R + block) * TB + half * TC
        return slopes.at[kk, pl.ds(pl.multiple_of(start, TC), TC), :]

    def sl_copy(a, j):
        _, kk, half, there, block = place(a, j)
        at = slope_at(dp, kk, block, half)
        to = (col + C - 1) % C if a == 0 else (col + 1) % C
        return copy(at, at, sl_s.at[a, j], sl_r.at[a, j], col=to)

    def xs_copy(a, j, e):
        _, kk, half, there, block = place(a, j)
        at = slope_at(dp, kk, block, half)
        return copy(at, at, xs_s.at[a, j, e - 1], xs_r.at[a, j, e - 1], dp=(dp + e) % D)

    lane = lax.broadcasted_iota(jnp.int32, (TC, 128), 1)

    def finish(a, i, pre):
        group, kk, half, there, block = place(a, i)
        sigma = jax.nn.sigmoid(pre)
        hid = pre * sigma
        head = heads[group * 2 + kk]
        value = jnp.sum(hid * head, axis=1, keepdims=True)
        at = pl.ds(pl.multiple_of(there * TB + half * TC, TC), TC)
        vals[at, :] += jnp.where(lane == group * 2 + kk, value, 0.0)

        @pl.when(group == 0)
        def _():
            hidden[kk, at, :] = hid.astype(bf16)
            start = (dp * R + block) * TB + half * TC
            slopes[kk, pl.ds(pl.multiple_of(start, TC), TC), :] = (
                head * (sigma * (1.0 + pre * (1.0 - sigma)))).astype(bf16)
            sl_copy(a, i).start()
            for e in range(1, D):
                xs_copy(a, i, e).start()

    vals[...] = jnp.zeros_like(vals)

    def step(s, carry):
        for a in range(2):
            far = col if a == 0 else C - 1 - col
            i = s - skew * far

            @pl.when((i >= 0) & (i < n))
            def _():
                prepare(a, i)
                group, kk, half, there, block = place(a, i)
                start = (jnp.where(group == 0, dp, D) * R + block) * TB + half * TC

                def partial():
                    left = emb[kk, pl.ds(pl.multiple_of(start, TC), TC), :]
                    return jnp.dot(left, w16[group * 2 + kk], preferred_element_type=f32)

                @pl.when(far == 0)
                def _():
                    rs_out[a, i] = partial().astype(bf16)
                    rs_copy(a, i).start()

                @pl.when((far > 0) & (far < C - 1))
                def _():
                    mine = partial()
                    rs_copy(a, i).wait_recv()
                    rs_out[a, i] = (mine + rs_in[a, i].astype(f32)).astype(bf16)
                    rs_copy(a, i).start()

                @pl.when(far == C - 1)
                def _():
                    mine = partial()
                    rs_copy(a, i).wait_recv()
                    finish(a, i, mine + rs_in[a, i].astype(f32))

            j = s - skew * (2 * (C - 1) - far)

            @pl.when((j >= 0) & (j < m) & (far < C - 1))
            def _():
                sl_copy(a, j).wait_recv()

                @pl.when(far > 0)
                def _():
                    sl_copy(a, j).start()
                for e in range(1, D):
                    xs_copy(a, j, e).start()
        return carry

    lax.fori_loop(0, n + skew * (C - 1), step, 0)

    def vt_copy(o):
        return copy(vt_own, vt_in.at[o - 1], vt_s.at[o - 1], vt_r.at[o - 1], row=(row + o) % R)

    def er_copy(x, a):
        c, d = plane[x]
        return copy(errs.at[dp, a], errs.at[dp, a], er_s.at[x], er_r.at[a, x],
                    col=(col + c) % C, dp=(dp + d) % D)

    def gh_copy(x, a):
        c, d = plane[x]
        return copy(gh.at[dp, a], gh.at[dp, a], gh_s.at[x], gh_r.at[a, x],
                    col=(col + c) % C, dp=(dp + d) % D)

    top = lax.broadcasted_iota(jnp.int32, (8, TB), 0)
    for a in range(2):
        @pl.when(col == (C - 1 if a == 0 else 0))
        def _():
            own = []
            for h in range(HI):
                seen = vals[h * TB:(h + 1) * TB, :] + tg_all[h * 2 + a][:, F + A:].astype(f32)
                own.append(seen.T[:8])
                vt_own[h] = own[h]
            for o in range(1, R):
                vt_copy(o).start()
            for o in range(1, R):
                vt_copy(o).wait()
            total = jnp.zeros((8, H), f32)
            for h in range(HI):
                summed = own[h]
                for o in range(1, R):
                    summed = summed + vt_in[o - 1, h]
                goal = own[h][4:5] + own[h][5:6] * jnp.minimum(summed[2:3], summed[3:4])
                err = jnp.where(top < 2, summed - goal, 0.0)
                errs[dp, a, h] = err
                twice = (2.0 * err).astype(bf16)
                for k in range(2):
                    got = jnp.dot(twice, hidden[k, h * TB:(h + 1) * TB, :],
                                  preferred_element_type=f32)
                    keep = lax.broadcasted_iota(jnp.int32, (8, H), 0) == k
                    total = total + jnp.where(keep, got, 0.0)
            for x in range(len(plane)):
                er_copy(x, a).start()
            gh[dp, a] = total
            for x in range(len(plane)):
                gh_copy(x, a).start()

    def late(s, carry):
        for a in range(2):
            far = col if a == 0 else C - 1 - col
            j = s - skew * (2 * (C - 1) - far)

            @pl.when((j >= 0) & (j < m) & (far < C - 1))
            def _():
                sl_copy(a, j).wait_recv()

                @pl.when(far > 0)
                def _():
                    sl_copy(a, j).start()
                for e in range(1, D):
                    xs_copy(a, j, e).start()
        return carry

    lax.fori_loop(n + skew * (C - 1), max(n + skew * (C - 1), m + 2 * skew * (C - 1)), late, 0)

    def pu_copy(o):
        return copy(pu_out.at[o], pu_in.at[o - 1], pu_s.at[o - 1], pu_r.at[o - 1],
                    row=(row + o) % R)

    def pz_copy(c):
        return copy(pz_all.at[col], pz_all.at[col], pz_s.at[c - 1], pz_r.at[c - 1],
                    col=(col + c) % C)

    lift = jnp.dot(a16[0], w16[0], preferred_element_type=f32).astype(bf16)
    last = (((1,), (1,)), ((), ()))
    first = (((0,), (0,)), ((), ()))
    own_push = None
    for o in range(R):
        got = lax.dot_general(slopes[0, rows_of(dp, (row + o) % R), :], lift, last,
                              preferred_element_type=f32)
        if o == 0:
            own_push = got
        else:
            pu_out[o] = got.astype(bf16)
            pu_copy(o).start()

    for e in range(1, D):
        src = (dp + D - e) % D
        for a in range(2):
            for o in range(HI):
                block = ((hi + o) % HI) * 2 + a
                xon_copy(a, o, block, e).wait_recv()
                embed_on(src, block)

    for o in range(1, R):
        pu_copy(o).wait_recv()
        own_push = own_push + pu_in[o - 1].astype(f32)
    pz_all[col] = own_push.astype(bf16)
    for c in range(1, C):
        pz_copy(c).start()

    for e in range(1, D):
        def take(j, carry):
            for a in range(2):
                xs_copy(a, j, e).wait_recv()
            return carry
        lax.fori_loop(0, m, take, 0)

    for a in range(2):
        end = C - 1 if a == 0 else 0
        for x, (c, d) in enumerate(plane):
            @pl.when((col + C - c) % C == end)
            def _():
                er_copy(x, a).wait_recv()

    epad[...] = jnp.zeros_like(epad)
    for d in range(D):
        for h in range(HI):
            for a in range(2):
                epad[0:8, :] = 2.0 * errs[d, a, h]
                at = slice((d * R + h * 2 + a) * TB, (d * R + h * 2 + a + 1) * TB)
                columns[at, :] = epad[...].T

    FR = F // R

    def ga_copy(o):
        to = (row + o) % R
        return copy(ga_out.at[to], ga_in.at[o - 1], ga_s.at[o - 1], ga_r.at[o - 1], row=to)

    def gb_copy(o):
        return copy(ga_all.at[row], ga_all.at[row], gb_s.at[o - 1], gb_r.at[o - 1],
                    row=(row + o) % R)

    for k in range(2):
        moved = jnp.zeros((A, H), f32)
        for d in range(D):
            for b in range(R):
                at = slice((d * R + b) * TB, (d * R + b + 1) * TB)
                scaled = columns[at, k:k + 1] * on_all[d, b][:, F:].astype(f32)
                moved = moved + lax.dot_general(scaled.astype(bf16), slopes[k, at, :], first,
                                                preferred_element_type=f32)
        term = lax.dot_general(moved.astype(bf16), w16[k], last, preferred_element_type=f32)
        for p in range(R):
            piece = term[:, p * FR:(p + 1) * FR]
            ga_own[p, k] = piece
            ga_out[p, k] = piece.astype(bf16)
    for o in range(1, R):
        ga_copy(o).start()

    def blend(fresh, target):
        return blend_rate * fresh + (1.0 - blend_rate) * target

    def grad_in(k):
        for b in range(D * R):
            at = slice(b * TB, (b + 1) * TB)
            scaled = columns[at, k:k + 1] * slopes[k, at, :].astype(f32)
            delta[k, at, :] = scaled.astype(bf16)

        def add(d, carry):
            at = pl.ds(pl.multiple_of(d * R * TB, R * TB), R * TB)
            new_in[k] += lax.dot_general(emb[k, at, :], delta[k, at, :], first,
                                         preferred_element_type=f32)
            return carry
        new_in[k] = lax.dot_general(emb[k, :R * TB, :], delta[k, :R * TB, :], first,
                                    preferred_element_type=f32)
        lax.fori_loop(1, D, add, 0)
        fresh = cin[k] - matrix_rate * new_in[k]
        new_in[k] = fresh
        new_tin[k] = blend(fresh, tin[k])

    grad_in(0)
    for o in range(1, R):
        ga_copy(o).wait_recv()
    for k in range(2):
        piece = ga_own[row, k]
        for o in range(1, R):
            piece = piece + ga_in[o - 1, k].astype(f32)
        ga_all[row, k] = piece.astype(bf16)
    for o in range(1, R):
        gb_copy(o).start()
    grad_in(1)

    for c in range(1, C):
        pz_copy(c).wait_recv()
    push = pz_all[0].astype(f32)
    for c in range(1, C):
        push = push + pz_all[c].astype(f32)
    push_out[...] = push * flag_column[...]
    errs_out[...] = errs[dp, lo, hi, 0:2, :]

    for a in range(2):
        end = C - 1 if a == 0 else 0
        for x, (c, d) in enumerate(plane):
            @pl.when((col + C - c) % C == end)
            def _():
                gh_copy(x, a).wait_recv()
    whole = gh[0, 0]
    for d in range(D):
        for a in range(2):
            if d or a:
                whole = whole + gh[d, a]
    new_head[...] = chead[...] - head_rate * whole[:2]
    new_thead[...] = blend(new_head[...], thead[...])

    for o in range(1, R):
        gb_copy(o).wait_recv()
    for p in range(R):
        for k in range(2):
            part = slice(p * FR, (p + 1) * FR)
            fresh = cact[k, :, part] - matrix_rate * ga_all[p, k].astype(f32)
            new_act[k, :, part] = fresh
            new_tact[k, :, part] = blend(fresh, tact[k, :, part])

    for o in range(HI):
        on_copy(o).wait_send()
        tg_copy(o).wait_send()
        if o > 0:
            fon_copy(o, row).wait_send()
            ftg_copy(o, row).wait_send()
        for a in range(2):
            for e in range(1, D):
                xon_copy(a, o, row, e).wait_send()
    for a in range(2):
        far = col if a == 0 else C - 1 - col

        @pl.when(far < C - 1)
        def _():
            def left(i, carry):
                rs_copy(a, i).wait_send()
                return carry
            lax.fori_loop(0, n, left, 0)

        @pl.when(far > 0)
        def _():
            def left(j, carry):
                sl_copy(a, j).wait_send()
                return carry
            lax.fori_loop(0, m, left, 0)

        def gone(j, carry):
            for e in range(1, D):
                xs_copy(a, j, e).wait_send()
            return carry
        lax.fori_loop(0, m, gone, 0)

        @pl.when(far == C - 1)
        def _():
            for x in range(len(plane)):
                er_copy(x, a).wait_send()
                gh_copy(x, a).wait_send()
    for o in range(1, R):
        pu_copy(o).wait_send()
        ga_copy(o).wait_send()
        gb_copy(o).wait_send()
    for c in range(1, C):
        pz_copy(c).wait_send()


def on_device(dims, observed, next_observed, actions, next_mean, policy_noise, rewards, discounts,
              actor_flags, critic_in, critic_act, critic_head, target_in, target_act, target_head):
    R, C, D, TB, F, H, A = dims
    HI, TC = R // 2, TB // 2
    n, m, planes = 8 * HI, 4 * HI, C * D - 1
    dma = lambda *shape: pltpu.SemaphoreType.DMA(shape)
    vmem = pltpu.VMEM
    scratch = [
        vmem((TB, F + A), bf16), vmem((TB, F + A + 128), bf16), vmem((4, 1, H), f32),
        vmem((TB, 1), f32), vmem((D * R * TB, 128), f32),
        vmem((4, F, H), bf16), vmem((4, A, F), bf16),
        vmem((D, R, TB, F + A), bf16), vmem((R, TB, F + A + 128), bf16),
        vmem((2, (D + 1) * R * TB, F), bf16),
        vmem((2, D * R * TB, H), bf16), vmem((2, D * R * TB, H), bf16),
        vmem((2, n, TC, H), bf16), vmem((2, n, TC, H), bf16),
        vmem((2, HI * TB, H), bf16), vmem((HI * TB, 128), f32),
        vmem((HI, 8, TB), f32), vmem((R - 1, HI, 8, TB), f32),
        vmem((D, 2, HI, 8, TB), f32), vmem((D, 2, 8, H), f32), vmem((128, TB), f32),
        vmem((R, 2, A, F // R), f32), vmem((R, 2, A, F // R), bf16),
        vmem((R - 1, 2, A, F // R), bf16), vmem((R, 2, A, F // R), bf16),
        vmem((R, TB, A), bf16), vmem((R - 1, TB, A), bf16), vmem((C, TB, A), bf16),
        dma(HI), dma(HI), dma(HI), dma(HI),
        dma(HI), dma(HI), dma(HI), dma(HI),
        dma(2, HI, D - 1), dma(2, HI, D - 1),
        dma(2, n), dma(2, n), dma(2, m), dma(2, m),
        dma(2, m, D - 1), dma(2, m, D - 1),
        dma(R - 1), dma(R - 1),
        dma(planes), dma(2, planes), dma(planes), dma(2, planes),
        dma(R - 1), dma(R - 1), dma(R - 1), dma(R - 1),
        dma(R - 1), dma(R - 1), dma(C - 1), dma(C - 1),
        vmem((TB, A), bf16), vmem((TB, A), f32), vmem((1, TB), bf16), vmem((1, TB), bf16),
        vmem((1, TB), jnp.int32), vmem((2, F, H), f32), vmem((2, A, F), f32), vmem((2, H), f32),
        vmem((2, F, H), f32), vmem((2, A, F), f32), vmem((2, H), f32), dma(16),
    ]
    spec = pl.BlockSpec(memory_space=vmem)
    results = (((2, F, H), f32), ((2, A, F), f32), ((2, H), f32), ((2, F, H), f32),
               ((2, A, F), f32), ((2, H), f32), ((2, TB), f32), ((TB, A), f32))
    kept = pl.pallas_call(
        functools.partial(kernel, dims),
        out_shape=tuple(vmem(shape, kind) for shape, kind in results),
        in_specs=[pl.BlockSpec(memory_space=pltpu.HBM)] * 14,
        out_specs=(spec,) * 8,
        scratch_shapes=scratch,
        compiler_params=pltpu.CompilerParams(
            collective_id=0, has_side_effects=True, vmem_limit_bytes=57 * 2 ** 20),
    )(*[pltpu.with_memory_space_constraint(one, pltpu.HBM) for one in (
        observed, next_observed, actions, next_mean, policy_noise, rewards[None, :],
        discounts[None, :], actor_flags[None, :], critic_in, critic_act, critic_head, target_in,
        target_act, target_head)])
    return pl.pallas_call(
        put_out,
        out_shape=tuple(jax.ShapeDtypeStruct(shape, kind) for shape, kind in results),
        in_specs=[spec] * 8,
        out_specs=(pl.BlockSpec(memory_space=pl.ANY),) * 8,
        scratch_shapes=[dma(8)],
        compiler_params=pltpu.CompilerParams(vmem_limit_bytes=12 * 2 ** 20),
    )(*[pltpu.with_memory_space_constraint(one, vmem) for one in kept])


def put_out(*refs):
    sems = refs[16]
    copies = [pltpu.make_async_copy(refs[x], refs[8 + x], sems.at[x]) for x in range(8)]
    for one in copies:
        one.start()
    for one in copies:
        one.wait()


def solution(mesh):
    def run(*args):
        R, C, D = mesh.shape["row"], mesh.shape["col"], mesh.shape["dp"]
        tokens, features = args[0].shape
        dims = (R, C, D, tokens // (R * D), features // C, args[8].shape[2] // R,
                args[2].shape[1])
        return sharded(dims)(*args)

    def sharded(dims):
        return jax.shard_map(
            functools.partial(on_device, dims),
            mesh=mesh,
            in_specs=(
                P(("row", "dp"), "col"),
                P(("row", "dp"), "col"),
                P(("row", "dp"), None),
                P(("row", "dp"), None),
                P(("row", "dp"), None),
                P(("row", "dp")),
                P(("row", "dp")),
                P(("row", "dp")),
                P(None, "col", "row"),
                P(None, None, "col"),
                P(None, "row"),
                P(None, "col", "row"),
                P(None, None, "col"),
                P(None, "row"),
            ),
            out_specs=(
                P(None, "col", "row"),
                P(None, None, "col"),
                P(None, "row"),
                P(None, "col", "row"),
                P(None, None, "col"),
                P(None, "row"),
                P(None, ("row", "dp")),
                P(("row", "dp"), None),
            ),
            check_vma=False,
        )

    return run
```

```python
import functools

import jax
import jax.numpy as jnp
from jax import lax
from jax.experimental import pallas as pl
from jax.experimental.pallas import tpu as pltpu
from jax.sharding import PartitionSpec as P

noise_clip = 0.5
matrix_rate = 0.004
head_rate = 0.0001
blend_rate = 0.005

f32 = jnp.float32
bf16 = jnp.bfloat16
skew = 3
pieces = 2


def kernel(dims, observed_at, next_observed_at, actions_at, next_mean_at, noise_at, rewards_at,
           discounts_at, flags_at, cin_at, cact_at, chead_at, tin_at, tact_at, thead_at,
           new_in, new_act, new_head, new_tin, new_tact, new_thead, errs_out, push_out,
           next_mean, noise, rewards, discounts, flags, cin, cact, chead, tin, tact, thead,
           on_own, tg_own, flag_column, w16, a16, on_all, tg_all, emb, slopes, delta, lift,
           t_out, t_in, o_out, o_in, hidden, vals_t, vals_o, rd_own, rd_all, vt_all, vo_all, gl,
           err_own, err_top, gh, epad, columns, scaled,
           ga_own, ga_out, ga_in, gb_all, gc_all, pu_out, pu_in, pz_all,
           load_s, on_s, on_r, tg_s, tg_r, ftg_s, ftg_r, ox_s, ox_r, oo_s, oo_r, rd_s, rd_r,
           tr_s, tr_r, or_s, or_r, xs_s, xs_r, vt_s, vt_r, vo_s, vo_r, gl_s, gl_r, er_s, er_r,
           gh_s, gh_r, ga_s, ga_r, gb_s, gb_r, gc_s, gc_r, pu_s, pu_r, pz_s, pz_r):
    R, C, D, TB, F, H, A = dims
    HI = R // 2
    TC = TB // pieces
    row, col, dp = lax.axis_index("row"), lax.axis_index("col"), lax.axis_index("dp")
    hi, lo = row // 2, row % 2
    nt = 2 * HI * pieces
    no = 2 * R * pieces
    partner = hi * 2 + (1 - lo)

    def copy(src, dst, ssem, rsem, **where):
        return pltpu.make_async_remote_copy(
            src_ref=src, dst_ref=dst, send_sem=ssem, recv_sem=rsem,
            device_id=where, device_id_type=pl.DeviceIdType.MESH)

    pairs = [(next_observed_at, tg_own.at[:, :F]), (next_mean_at, next_mean), (noise_at, noise),
             (tact_at, tact), (tin_at.at[0], tin.at[0]), (tin_at.at[1], tin.at[1]),
             (thead_at, thead), (observed_at, on_own.at[:, :F]), (actions_at, on_own.at[:, F:]),
             (rewards_at, rewards), (discounts_at, discounts), (flags_at, flags),
             (cact_at, cact), (cin_at.at[0], cin.at[0]), (cin_at.at[1], cin.at[1]),
             (chead_at, chead)]
    loads = [pltpu.make_async_copy(src, dst, load_s.at[x]) for x, (src, dst) in enumerate(pairs)]
    for load in loads:
        load.start()

    plane = [(c, d) for d in range(D) for c in range(C) if c or d]
    group = [(r, d) for d in range(D) for r in range(R) if r or d]
    others = [(r, 0, d) for r, d in group] + [(0, c, d) for c, d in plane if c]
    barrier = pltpu.get_barrier_semaphore()
    for r, c, d in others:
        pl.semaphore_signal(barrier, inc=1,
                            device_id={"row": (row + r) % R, "col": (col + c) % C,
                                       "dp": (dp + d) % D},
                            device_id_type=pl.DeviceIdType.MESH)

    vals_t[...] = jnp.zeros_like(vals_t)
    vals_o[...] = jnp.zeros_like(vals_o)
    for x in range(3):
        loads[x].wait()
    tg_own[:, F:] = jnp.clip(
        next_mean[...].astype(f32) + jnp.clip(noise[...], -noise_clip, noise_clip), -1.0, 1.0
    ).astype(bf16)
    pl.semaphore_wait(barrier, len(others))

    def tg_copy(o):
        to = partner if o == 0 else ((hi + o) % HI) * 2 + lo
        return copy(tg_own, tg_all.at[row], tg_s.at[o], tg_r.at[o], row=to)

    def ftg_copy(o, block):
        return copy(tg_all.at[block], tg_all.at[block], ftg_s.at[o], ftg_r.at[o], row=partner)

    def on_copy(o):
        return copy(on_own, on_all.at[dp, row], on_s.at[o - 1], on_r.at[o - 1],
                    row=(row + o) % R)

    def ox_copy(e):
        return copy(on_own, on_all.at[dp, row], ox_s.at[e - 1], ox_r.at[e - 1], dp=(dp + e) % D)

    def oo_copy(e, o):
        at = on_all.at[(dp + D - e) % D, row]
        return copy(at, at, oo_s.at[e - 1, o - 1], oo_r.at[e - 1, o - 1], row=(row + o) % R)

    def rd_copy(o):
        return copy(rd_own, rd_all.at[row], rd_s.at[o - 1], rd_r.at[o - 1], row=(row + o) % R)

    for o in range(HI):
        tg_copy(o).start()
    tg_all[row] = tg_own[...]
    for x in range(3, 7):
        loads[x].wait()
    for k in range(2):
        a16[2 + k] = tact[k].astype(bf16)
        w16[2 + k] = tin[k].astype(bf16)
    for x in range(7, 12):
        loads[x].wait()
    for e in range(1, D):
        ox_copy(e).start()
    rd_own[...] = jnp.zeros_like(rd_own)
    rd_own[0:1, :] = rewards[...].astype(f32)
    rd_own[1:2, :] = discounts[...].astype(f32)
    for o in range(1, R):
        on_copy(o).start()
        rd_copy(o).start()
    on_all[dp, row] = on_own[...]
    rd_all[row] = rd_own[...]

    def rows_of(d, block):
        return pl.ds(pl.multiple_of((d * R + block) * TB, TB), TB)

    def embed_on(d, block):
        x = on_all[d, block]
        for k in range(2):
            mixed = jnp.dot(x[:, F:], a16[k], preferred_element_type=f32)
            emb[k, rows_of(d, block), :] = (x[:, :F].astype(f32) + mixed).astype(bf16)

    def embed_tg(block):
        x = tg_all[block]
        for k in range(2):
            mixed = jnp.dot(x[:, F:], a16[2 + k], preferred_element_type=f32)
            emb[k, rows_of(D, block), :] = (x[:, :F].astype(f32) + mixed).astype(bf16)

    def prepare_tg(a, i):
        for o in range(HI):
            block = ((hi + HI - o) % HI) * 2 + a

            @pl.when(i == 2 * pieces * o)
            def _():
                @pl.when(lo == a)
                def _():
                    if o > 0:
                        tg_copy(o).wait_recv()
                        ftg_copy(o, block).start()

                @pl.when(lo != a)
                def _():
                    if o > 0:
                        ftg_copy(o, block).wait_recv()
                    else:
                        tg_copy(0).wait_recv()
                embed_tg(block)

    def prepare_on(q):
        for o in range(R):
            @pl.when(q == 2 * pieces * o)
            def _():
                if o > 0:
                    on_copy(o).wait_recv()
                embed_on(dp, (row + R - o) % R)

    def along(a):
        return (col + 1) % C if a == 0 else (col + C - 1) % C

    def tr_copy(a, i):
        return copy(t_out.at[a, i], t_in.at[a, i], tr_s.at[a, i], tr_r.at[a, i], col=along(a))

    def or_copy(a, q):
        return copy(o_out.at[a, q], o_in.at[a, q], or_s.at[a, q], or_r.at[a, q], col=along(a))

    def place_t(a, i):
        block = ((hi + HI - i // (2 * pieces)) % HI) * 2 + a
        return block, (i // pieces) % 2, i % pieces

    def place_o(q):
        return (row + R - q // (2 * pieces)) % R, (q // pieces) % 2, q % pieces

    def chunk(d, block, piece):
        return pl.ds(pl.multiple_of((d * R + block) * TB + piece * TC, TC), TC)

    def xs_copy(q, e):
        block, kk, piece = place_o(q)
        at = slopes.at[kk, chunk(dp, block, piece), :]
        return copy(at, at, xs_s.at[q, e - 1], xs_r.at[q, e - 1], dp=(dp + e) % D)

    def vt_copy(o):
        return copy(vt_all.at[row], vt_all.at[row], vt_s.at[o - 1], vt_r.at[o - 1],
                    row=(row + o) % R)

    def gl_copy(x, a):
        c, d = plane[x]
        return copy(gl.at[dp, a], gl.at[dp, a], gl_s.at[x], gl_r.at[a, x],
                    col=(col + c) % C, dp=(dp + d) % D)

    def vo_copy(x):
        r, d = group[x]
        return copy(vo_all.at[dp, row], vo_all.at[dp, row], vo_s.at[x], vo_r.at[x],
                    row=(row + r) % R, dp=(dp + d) % D)

    lane = lax.broadcasted_iota(jnp.int32, (TC, 128), 1)

    def note(store, block, kk, piece, gate, head):
        value = jnp.sum(gate * head, axis=1, keepdims=True)
        at = pl.ds(pl.multiple_of(piece * TC, TC), TC)
        store[at, :] += jnp.where(lane == kk * R + block, value, 0.0)

    def finish_t(a, i, pre):
        block, kk, piece = place_t(a, i)
        note(vals_t, block, kk, piece, pre * jax.nn.sigmoid(pre), thead[pl.ds(kk, 1), :])

    def finish_o(q, pre):
        block, kk, piece = place_o(q)
        sigma = jax.nn.sigmoid(pre)
        gate = pre * sigma
        head = chead[pl.ds(kk, 1), :]
        slopes[kk, chunk(dp, block, piece), :] = (
            head * (sigma * (1.0 + pre * (1.0 - sigma)))).astype(bf16)
        for e in range(1, D):
            xs_copy(q, e).start()
        hidden[kk, chunk(0, block, piece), :] = gate.astype(bf16)
        note(vals_o, block, kk, piece, gate, head)

    def settle(a, i):
        @pl.when(i == nt)
        def _():
            vt_all[row] = vals_t[...].T[:2 * R]
            for o in range(1, R):
                vt_copy(o).start()

        @pl.when(i == nt + 3)
        def _():
            for o in range(1, R):
                vt_copy(o).wait_recv()
            total = vt_all[0]
            for r in range(1, R):
                total = total + vt_all[r]
            reward = jnp.concatenate([rd_all[b, 0:1] for b in range(R)], axis=0)
            discount = jnp.concatenate([rd_all[b, 1:2] for b in range(R)], axis=0)
            goal = reward + discount * jnp.minimum(total[:R], total[R:])
            mine = lax.broadcasted_iota(jnp.int32, (R, TB), 0) % 2 == a
            goal = jnp.where(mine, goal, 0.0)
            gl[dp, a] = jnp.concatenate([goal, goal], axis=0)
            for x in range(len(plane)):
                gl_copy(x, a).start()

    steps = nt + no + skew * (C - 1)

    def aside(s):
        @pl.when(s == 1)
        def _():
            for x in range(12, 16):
                loads[x].wait()
            for k in range(2):
                a16[k] = cact[k].astype(bf16)
                w16[k] = cin[k].astype(bf16)

        @pl.when(s == 4)
        def _():
            for o in range(1, R):
                rd_copy(o).wait_recv()

        @pl.when(s == nt)
        def _():
            for e in range(1, D):
                ox_copy(e).wait_recv()
                for o in range(1, R):
                    oo_copy(e, o).start()

        @pl.when(s == nt + 1)
        def _():
            lift[...] = jnp.dot(a16[0], w16[0], preferred_element_type=f32).astype(bf16)

        for e in range(1, D):
            for o in range(R):
                @pl.when(s == nt + no // 2 + (e - 1) * R + o)
                def _():
                    if o > 0:
                        oo_copy(e, o).wait_recv()
                    embed_on((dp + D - e) % D, (row + R - o) % R)

    def step(s, carry):
        for a in range(2):
            far = col if a == 0 else C - 1 - col
            i = s - skew * far

            @pl.when((i >= 0) & (i < nt))
            def _():
                prepare_tg(a, i)
                block, kk, piece = place_t(a, i)

                def partial():
                    return jnp.dot(emb[kk, chunk(D, block, piece), :], w16[2 + kk],
                                   preferred_element_type=f32)

                @pl.when(far == 0)
                def _():
                    t_out[a, i] = partial().astype(bf16)
                    tr_copy(a, i).start()

                @pl.when((far > 0) & (far < C - 1))
                def _():
                    mine = partial()
                    tr_copy(a, i).wait_recv()
                    t_out[a, i] = (mine + t_in[a, i].astype(f32)).astype(bf16)
                    tr_copy(a, i).start()

                @pl.when(far == C - 1)
                def _():
                    mine = partial()
                    tr_copy(a, i).wait_recv()
                    finish_t(a, i, mine + t_in[a, i].astype(f32))

            @pl.when((i >= nt) & (i < nt + no))
            def _():
                q = i - nt
                block, kk, piece = place_o(q)
                later = 2 * far > C - 1 if a == 0 else 2 * far >= C - 1

                @pl.when(jnp.logical_not(later))
                def _():
                    prepare_on(q)

                def partial():
                    return jnp.dot(emb[kk, chunk(dp, block, piece), :], w16[kk],
                                   preferred_element_type=f32)

                @pl.when(far == 0)
                def _():
                    o_out[a, q] = partial().astype(bf16)
                    or_copy(a, q).start()

                @pl.when((far > 0) & (far < C - 1))
                def _():
                    mine = partial()
                    or_copy(a, q).wait_recv()
                    mine = mine + o_in[a, q].astype(f32)
                    o_out[a, q] = mine.astype(bf16)
                    or_copy(a, q).start()

                    @pl.when(later)
                    def _():
                        finish_o(q, mine + o_in[1 - a, q].astype(f32))

                @pl.when(far == C - 1)
                def _():
                    mine = partial()
                    or_copy(a, q).wait_recv()
                    finish_o(q, mine + o_in[a, q].astype(f32))

            @pl.when(far == C - 1)
            def _():
                settle(a, i)
        aside(s)
        return carry

    lax.fori_loop(0, steps, step, 0)

    vo_all[dp, row] = vals_o[...].T[:2 * R]
    for x in range(len(group)):
        vo_copy(x).start()

    def pu_copy(o):
        return copy(pu_out.at[o - 1], pu_in.at[o - 1], pu_s.at[o - 1], pu_r.at[o - 1],
                    row=(row + o) % R)

    def pz_copy(c):
        return copy(pz_all.at[col], pz_all.at[col], pz_s.at[c - 1], pz_r.at[c - 1],
                    col=(col + c) % C)

    last = (((1,), (1,)), ((), ()))
    first = (((0,), (0,)), ((), ()))
    own_push = None
    for o in list(range(1, R)) + [0]:
        got = lax.dot_general(slopes[0, rows_of(dp, (row + o) % R), :], lift[...], last,
                              preferred_element_type=f32)
        if o == 0:
            own_push = got
        else:
            pu_out[o - 1] = got.astype(bf16)
            pu_copy(o).start()

    for a in range(2):
        end = C - 1 if a == 0 else 0
        for x, (c, d) in enumerate(plane):
            @pl.when((col + C - c) % C == end)
            def _():
                gl_copy(x, a).wait_recv()

    for o in range(1, R):
        pu_copy(o).wait_recv()
        own_push = own_push + pu_in[o - 1].astype(f32)
    pz_all[col] = own_push.astype(bf16)
    for c in range(1, C):
        pz_copy(c).start()

    for e in range(1, D):
        def take(q, carry):
            xs_copy(q, e).wait_recv()
            return carry
        lax.fori_loop(0, no, take, 0)
    for x in range(len(group)):
        vo_copy(x).wait_recv()

    epad[...] = jnp.zeros_like(epad)
    for d in range(D):
        value = vo_all[d, 0]
        for r in range(1, R):
            value = value + vo_all[d, r]
        err = value - (gl[d, 0] + gl[d, 1])
        err_own[d] = err
        epad[:2 * R, :] = 2.0 * err
        columns[d] = epad[...].T

    F2 = F // 2

    def ga_copy(k):
        return copy(ga_out.at[k], ga_in.at[k], ga_s.at[k], ga_r.at[k], row=partner)

    def gb_copy(k, o):
        return copy(gb_all.at[k, hi], gb_all.at[k, hi], gb_s.at[k, o - 1], gb_r.at[k, o - 1],
                    row=((hi + o) % HI) * 2 + lo)

    def gc_copy(k):
        return copy(gc_all.at[k, lo], gc_all.at[k, lo], gc_s.at[k], gc_r.at[k], row=partner)

    for k in range(2):
        moved = jnp.zeros((A, H), f32)
        for d in range(D):
            for b in range(R):
                scaled[b * TB:(b + 1) * TB, :] = (
                    columns[d, :, k * R + b:k * R + b + 1] * on_all[d, b][:, F:].astype(f32)
                ).astype(bf16)
            moved = moved + lax.dot_general(
                scaled[...], slopes[k, d * R * TB:(d + 1) * R * TB, :], first,
                preferred_element_type=f32)
        term = lax.dot_general(moved.astype(bf16), w16[k], last, preferred_element_type=f32)

        @pl.when(lo == 0)
        def _():
            ga_own[k] = term[:, :F2]
            ga_out[k] = term[:, F2:].astype(bf16)

        @pl.when(lo == 1)
        def _():
            ga_own[k] = term[:, F2:]
            ga_out[k] = term[:, :F2].astype(bf16)
        ga_copy(k).start()

    def er_copy(c):
        return copy(err_top, err_top, er_s.at[c - 1], er_r.at[c - 1], col=(col + c) % C)

    def gh_copy(x):
        c, d = plane[x]
        return copy(gh.at[dp], gh.at[dp], gh_s.at[x], gh_r.at[x],
                    col=(col + c) % C, dp=(dp + d) % D)

    slot = lax.broadcasted_iota(jnp.int32, (2 * R, H), 0)

    @pl.when(col == 0)
    def _():
        err_top[...] = err_own[dp]
        for c in range(1, C):
            er_copy(c).start()
        twice = (2.0 * err_own[dp]).astype(bf16)
        total = jnp.zeros((2 * R, H), f32)
        for k in range(2):
            for b in range(R):
                got = jnp.dot(twice, hidden[k, b * TB:(b + 1) * TB, :],
                              preferred_element_type=f32)
                total = total + jnp.where(slot == k * R + b, got, 0.0)
        gh[dp] = total
        for x in range(len(plane)):
            gh_copy(x).start()

    for k in range(2):
        ga_copy(k).wait_recv()
        gb_all[k, hi] = (ga_own[k] + ga_in[k].astype(f32)).astype(bf16)
        for o in range(1, HI):
            gb_copy(k, o).start()

    def blend(fresh, target):
        return blend_rate * fresh + (1.0 - blend_rate) * target

    def grad_in(k):
        def scale(d):
            for b in range(R):
                at = pl.ds(pl.multiple_of((d * R + b) * TB, TB), TB)
                delta[b * TB:(b + 1) * TB, :] = (
                    columns[d, :, k * R + b:k * R + b + 1] * slopes[k, at, :].astype(f32)
                ).astype(bf16)
            at = pl.ds(pl.multiple_of(d * R * TB, R * TB), R * TB)
            return lax.dot_general(emb[k, at, :], delta[...], first, preferred_element_type=f32)

        def add(d, carry):
            new_in[k] += scale(d)
            return carry
        new_in[k] = scale(0)
        lax.fori_loop(1, D, add, 0)
        fresh = cin[k] - matrix_rate * new_in[k]
        new_in[k] = fresh
        new_tin[k] = blend(fresh, tin[k])

    grad_in(0)
    grad_in(1)

    for k in range(2):
        for o in range(1, HI):
            gb_copy(k, o).wait_recv()
        piece = gb_all[k, 0].astype(f32)
        for h in range(1, HI):
            piece = piece + gb_all[k, h].astype(f32)
        gc_all[k, lo] = piece.astype(bf16)
        gc_copy(k).start()

    for c in range(1, C):
        pz_copy(c).wait_recv()
    push = pz_all[0].astype(f32)
    for c in range(1, C):
        push = push + pz_all[c].astype(f32)
    epad[0:1, :] = flags[...].astype(f32)
    flag_column[...] = epad[...].T[:, 0:1]
    push_out[...] = push * flag_column[...]

    for c in range(1, C):
        @pl.when(col == c)
        def _():
            er_copy(c).wait_recv()
    for k in range(2):
        errs_out[k:k + 1, :] = err_top[pl.ds(k * R + row, 1), :]

    for x, (c, d) in enumerate(plane):
        @pl.when(col == c)
        def _():
            gh_copy(x).wait_recv()
    whole = gh[0]
    for d in range(1, D):
        whole = whole + gh[d]
    for k in range(2):
        grad = jnp.sum(whole[k * R:(k + 1) * R], axis=0, keepdims=True)
        fresh = chead[k:k + 1, :] - head_rate * grad
        new_head[k:k + 1, :] = fresh
        new_thead[k:k + 1, :] = blend(fresh, thead[k:k + 1, :])

    for k in range(2):
        gc_copy(k).wait_recv()
        for p in range(2):
            part = slice(p * F2, (p + 1) * F2)
            fresh = cact[k, :, part] - matrix_rate * gc_all[k, p].astype(f32)
            new_act[k, :, part] = fresh
            new_tact[k, :, part] = blend(fresh, tact[k, :, part])

    for o in range(HI):
        tg_copy(o).wait_send()
        if o > 0:
            ftg_copy(o, row).wait_send()
    for o in range(1, R):
        on_copy(o).wait_send()
        rd_copy(o).wait_send()
        pu_copy(o).wait_send()
        for e in range(1, D):
            oo_copy(e, o).wait_send()
    for e in range(1, D):
        ox_copy(e).wait_send()
    for a in range(2):
        far = col if a == 0 else C - 1 - col

        @pl.when(far < C - 1)
        def _():
            def left(i, carry):
                tr_copy(a, i).wait_send()
                return carry
            lax.fori_loop(0, nt, left, 0)

            def gone(q, carry):
                or_copy(a, q).wait_send()
                return carry
            lax.fori_loop(0, no, gone, 0)

        @pl.when(far == C - 1)
        def _():
            for o in range(1, R):
                vt_copy(o).wait_send()
            for x in range(len(plane)):
                gl_copy(x, a).wait_send()

    def away(q, carry):
        for e in range(1, D):
            xs_copy(q, e).wait_send()
        return carry
    lax.fori_loop(0, no, away, 0)
    for x in range(len(group)):
        vo_copy(x).wait_send()
    for c in range(1, C):
        pz_copy(c).wait_send()

    @pl.when(col == 0)
    def _():
        for c in range(1, C):
            er_copy(c).wait_send()
        for x in range(len(plane)):
            gh_copy(x).wait_send()
    for k in range(2):
        ga_copy(k).wait_send()
        gc_copy(k).wait_send()
        for o in range(1, HI):
            gb_copy(k, o).wait_send()


def put_out(*refs):
    count = len(refs) // 2
    copies = [pltpu.make_async_copy(refs[x], refs[count + x], refs[-1].at[x])
              for x in range(count)]
    for one in copies:
        one.start()
    for one in copies:
        one.wait()


def on_device(dims, observed, next_observed, actions, next_mean, policy_noise, rewards, discounts,
              actor_flags, critic_in, critic_act, critic_head, target_in, target_act, target_head):
    R, C, D, TB, F, H, A = dims
    HI, TC = R // 2, TB // pieces
    nt, no = 2 * HI * pieces, 2 * R * pieces
    planes, groups = C * D - 1, R * D - 1
    dma = lambda *shape: pltpu.SemaphoreType.DMA(shape)
    vmem = pltpu.VMEM
    scratch = [
        vmem((TB, A), bf16), vmem((TB, A), f32), vmem((1, TB), bf16), vmem((1, TB), bf16),
        vmem((1, TB), jnp.int32), vmem((2, F, H), f32), vmem((2, A, F), f32), vmem((2, H), f32),
        vmem((2, F, H), f32), vmem((2, A, F), f32), vmem((2, H), f32),
        vmem((TB, F + A), bf16), vmem((TB, F + A), bf16), vmem((TB, 1), f32),
        vmem((4, F, H), bf16), vmem((4, A, F), bf16),
        vmem((D, R, TB, F + A), bf16), vmem((R, TB, F + A), bf16),
        vmem((2, (D + 1) * R * TB, F), bf16),
        vmem((2, D * R * TB, H), bf16), vmem((R * TB, H), bf16), vmem((A, H), bf16),
        vmem((2, nt, TC, H), bf16), vmem((2, nt, TC, H), bf16),
        vmem((2, no, TC, H), bf16), vmem((2, no, TC, H), bf16),
        vmem((2, R * TB, H), bf16), vmem((TB, 128), f32), vmem((TB, 128), f32),
        vmem((8, TB), f32), vmem((R, 8, TB), f32), vmem((R, 2 * R, TB), f32),
        vmem((D, R, 2 * R, TB), f32), vmem((D, 2, 2 * R, TB), f32),
        vmem((D, 2 * R, TB), f32), vmem((2 * R, TB), f32), vmem((D, 2 * R, H), f32),
        vmem((128, TB), f32), vmem((D, TB, 128), f32), vmem((R * TB, A), bf16),
        vmem((2, A, F // 2), f32), vmem((2, A, F // 2), bf16), vmem((2, A, F // 2), bf16),
        vmem((2, HI, A, F // 2), bf16), vmem((2, 2, A, F // 2), bf16),
        vmem((R - 1, TB, A), bf16), vmem((R - 1, TB, A), bf16), vmem((C, TB, A), bf16),
        dma(16),
        dma(R - 1), dma(R - 1), dma(HI), dma(HI), dma(HI), dma(HI),
        dma(D - 1), dma(D - 1), dma(D - 1, R - 1), dma(D - 1, R - 1), dma(R - 1), dma(R - 1),
        dma(2, nt), dma(2, nt), dma(2, no), dma(2, no), dma(no, D - 1), dma(no, D - 1),
        dma(R - 1), dma(R - 1), dma(groups), dma(groups), dma(planes), dma(2, planes),
        dma(C - 1), dma(C - 1), dma(planes), dma(planes),
        dma(2), dma(2), dma(2, HI - 1), dma(2, HI - 1), dma(2), dma(2),
        dma(R - 1), dma(R - 1), dma(C - 1), dma(C - 1),
    ]
    spec = pl.BlockSpec(memory_space=vmem)
    results = (((2, F, H), f32), ((2, A, F), f32), ((2, H), f32), ((2, F, H), f32),
               ((2, A, F), f32), ((2, H), f32), ((2, TB), f32), ((TB, A), f32))
    kept = pl.pallas_call(
        functools.partial(kernel, dims),
        out_shape=tuple(vmem(shape, kind) for shape, kind in results),
        in_specs=[pl.BlockSpec(memory_space=pltpu.HBM)] * 14,
        out_specs=(spec,) * len(results),
        scratch_shapes=scratch,
        compiler_params=pltpu.CompilerParams(
            collective_id=0, has_side_effects=True, vmem_limit_bytes=57 * 2 ** 20),
    )(*[pltpu.with_memory_space_constraint(one, pltpu.HBM) for one in (
        observed, next_observed, actions, next_mean, policy_noise, rewards[None, :],
        discounts[None, :], actor_flags[None, :], critic_in, critic_act, critic_head, target_in,
        target_act, target_head)])
    return pl.pallas_call(
        put_out,
        out_shape=tuple(jax.ShapeDtypeStruct(shape, kind) for shape, kind in results),
        in_specs=[spec] * len(results),
        out_specs=(pl.BlockSpec(memory_space=pl.ANY),) * len(results),
        scratch_shapes=[dma(len(results))],
        compiler_params=pltpu.CompilerParams(vmem_limit_bytes=12 * 2 ** 20),
    )(*[pltpu.with_memory_space_constraint(one, vmem) for one in kept])


def solution(mesh):
    def run(*args):
        R, C, D = mesh.shape["row"], mesh.shape["col"], mesh.shape["dp"]
        tokens, features = args[0].shape
        dims = (R, C, D, tokens // (R * D), features // C, args[8].shape[2] // R,
                args[2].shape[1])
        return sharded(dims)(*args)

    def sharded(dims):
        return jax.shard_map(
            functools.partial(on_device, dims),
            mesh=mesh,
            in_specs=(
                P(("row", "dp"), "col"),
                P(("row", "dp"), "col"),
                P(("row", "dp"), None),
                P(("row", "dp"), None),
                P(("row", "dp"), None),
                P(("row", "dp")),
                P(("row", "dp")),
                P(("row", "dp")),
                P(None, "col", "row"),
                P(None, None, "col"),
                P(None, "row"),
                P(None, "col", "row"),
                P(None, None, "col"),
                P(None, "row"),
            ),
            out_specs=(
                P(None, "col", "row"),
                P(None, None, "col"),
                P(None, "row"),
                P(None, "col", "row"),
                P(None, None, "col"),
                P(None, "row"),
                P(None, ("row", "dp")),
                P(("row", "dp"), None),
            ),
            check_vma=False,
        )

    return run
```

```python
import functools

import jax
import jax.numpy as jnp
from jax import lax
from jax.experimental import pallas as pl
from jax.experimental.pallas import tpu as pltpu
from jax.sharding import PartitionSpec as P

noise_clip = 0.5
matrix_rate = 0.004
head_rate = 0.0001
blend_rate = 0.005

f32 = jnp.float32
bf16 = jnp.bfloat16
skew = 3
lead = 2
pieces = 2


def kernel(dims, observed_at, next_observed_at, actions_at, next_mean_at, noise_at, rewards_at,
           discounts_at, flags_at, cin_at, cact_at, chead_at, tin_at, tact_at, thead_at,
           new_in, new_act, new_head, new_tin, new_tact, new_thead, errs_out, push_out,
           next_mean, noise, rewards, discounts, flags, cin, cact, chead, tin, tact, thead,
           on_own, tg_own, flag_column, w16, a16, on_all, tg_all, emb, slopes, delta, lift,
           sums_out, sums_in, mine, hidden, vals_t, vals_o, rd_own, rd_all, vt_all, vo_all, gl,
           err_own, err_top, gh, epad, columns, scaled,
           ga_own, ga_out, ga_in, gb_all, gc_all, pu_out, pu_in, pz_all,
           load_s, on_s, on_r, tg_s, tg_r, ftg_s, ftg_r, ox_s, ox_r, oo_s, oo_r, rd_s, rd_r,
           sm_s, sm_r, xs_s, xs_r, vt_s, vt_r, vo_s, vo_r, gl_s, gl_r, er_s, er_r,
           gh_s, gh_r, ga_s, ga_r, gb_s, gb_r, gc_s, gc_r, pu_s, pu_r, pz_s, pz_r):
    R, C, D, TB, F, H, A = dims
    HI = R // 2
    TC = TB // pieces
    row, col, dp = lax.axis_index("row"), lax.axis_index("col"), lax.axis_index("dp")
    hi, lo = row // 2, row % 2
    nt = 2 * HI * pieces
    no = 2 * R * pieces
    n = nt + no
    partner = hi * 2 + (1 - lo)

    def copy(src, dst, ssem, rsem, **where):
        return pltpu.make_async_remote_copy(
            src_ref=src, dst_ref=dst, send_sem=ssem, recv_sem=rsem,
            device_id=where, device_id_type=pl.DeviceIdType.MESH)

    pairs = [(next_observed_at, tg_own.at[:, :F]), (next_mean_at, next_mean), (noise_at, noise),
             (tact_at, tact), (tin_at.at[0], tin.at[0]), (tin_at.at[1], tin.at[1]),
             (thead_at, thead), (observed_at, on_own.at[:, :F]), (actions_at, on_own.at[:, F:]),
             (rewards_at, rewards), (discounts_at, discounts), (flags_at, flags),
             (cact_at, cact), (cin_at.at[0], cin.at[0]), (cin_at.at[1], cin.at[1]),
             (chead_at, chead)]
    loads = [pltpu.make_async_copy(src, dst, load_s.at[x]) for x, (src, dst) in enumerate(pairs)]
    for load in loads:
        load.start()

    plane = [(c, d) for d in range(D) for c in range(C) if c or d]
    group = [(r, d) for d in range(D) for r in range(R) if r or d]
    others = [(r, 0, d) for r, d in group] + [(0, c, d) for c, d in plane if c]
    barrier = pltpu.get_barrier_semaphore()
    for r, c, d in others:
        pl.semaphore_signal(barrier, inc=1,
                            device_id={"row": (row + r) % R, "col": (col + c) % C,
                                       "dp": (dp + d) % D},
                            device_id_type=pl.DeviceIdType.MESH)

    vals_t[...] = jnp.zeros_like(vals_t)
    vals_o[...] = jnp.zeros_like(vals_o)
    for x in range(3):
        loads[x].wait()
    tg_own[:, F:] = jnp.clip(
        next_mean[...].astype(f32) + jnp.clip(noise[...], -noise_clip, noise_clip), -1.0, 1.0
    ).astype(bf16)
    pl.semaphore_wait(barrier, len(others))

    def tg_copy(o):
        to = partner if o == 0 else ((hi + o) % HI) * 2 + lo
        return copy(tg_own, tg_all.at[row], tg_s.at[o], tg_r.at[o], row=to)

    def ftg_copy(o, block):
        return copy(tg_all.at[block], tg_all.at[block], ftg_s.at[o], ftg_r.at[o], row=partner)

    def on_copy(o):
        return copy(on_own, on_all.at[dp, row], on_s.at[o - 1], on_r.at[o - 1],
                    row=(row + o) % R)

    def ox_copy(e):
        return copy(on_own, on_all.at[dp, row], ox_s.at[e - 1], ox_r.at[e - 1], dp=(dp + e) % D)

    def oo_copy(e, o):
        at = on_all.at[(dp + D - e) % D, row]
        return copy(at, at, oo_s.at[e - 1, o - 1], oo_r.at[e - 1, o - 1], row=(row + o) % R)

    def rd_copy(o):
        return copy(rd_own, rd_all.at[row], rd_s.at[o - 1], rd_r.at[o - 1], row=(row + o) % R)

    for o in range(HI):
        tg_copy(o).start()
    tg_all[row] = tg_own[...]
    for x in range(9, 11):
        loads[x].wait()
    rd_own[...] = jnp.zeros_like(rd_own)
    rd_own[0:1, :] = rewards[...].astype(f32)
    rd_own[1:2, :] = discounts[...].astype(f32)
    for o in range(1, R):
        rd_copy(o).start()
    rd_all[row] = rd_own[...]
    for x in range(3, 7):
        loads[x].wait()
    for k in range(2):
        a16[2 + k] = tact[k].astype(bf16)
        w16[2 + k] = tin[k].astype(bf16)
    for x in (7, 8):
        loads[x].wait()
    for e in range(1, D):
        ox_copy(e).start()
    for o in range(1, R):
        on_copy(o).start()
    on_all[dp, row] = on_own[...]

    def rows_of(d, block):
        return pl.ds(pl.multiple_of((d * R + block) * TB, TB), TB)

    def embed_on(d, block):
        x = on_all[d, block]
        for k in range(2):
            mixed = jnp.dot(x[:, F:], a16[k], preferred_element_type=f32)
            emb[k, rows_of(d, block), :] = (x[:, :F].astype(f32) + mixed).astype(bf16)

    def embed_tg(block):
        x = tg_all[block]
        for k in range(2):
            mixed = jnp.dot(x[:, F:], a16[2 + k], preferred_element_type=f32)
            emb[k, rows_of(D, block), :] = (x[:, :F].astype(f32) + mixed).astype(bf16)

    def prepare_tg(a, i):
        for o in range(HI):
            block = ((hi + HI - o) % HI) * 2 + a

            @pl.when(i == 2 * pieces * o)
            def _():
                @pl.when(lo != a)
                def _():
                    if o > 0:
                        ftg_copy(o, block).wait_recv()
                    else:
                        tg_copy(0).wait_recv()
                embed_tg(block)

    def forward_tg(a, i):
        for o in range(1, HI):
            @pl.when((i == 2 * pieces * o - 1) & (lo == a))
            def _():
                tg_copy(o).wait_recv()
                ftg_copy(o, ((hi + HI - o) % HI) * 2 + a).start()

    def prepare_on(q):
        for o in range(R):
            @pl.when(q == 2 * pieces * o)
            def _():
                if o > 0:
                    on_copy(o).wait_recv()
                embed_on(dp, (row + R - o) % R)

    def along(a):
        return (col + 1) % C if a == 0 else (col + C - 1) % C

    def sm_copy(a, i):
        return copy(sums_out.at[a, i], sums_in.at[a, i], sm_s.at[a], sm_r.at[a, i], col=along(a))

    def sm_sent(a):
        return copy(sums_out.at[a], sums_in.at[a], sm_s.at[a], sm_r.at[a, 0], col=along(a))

    def place_t(a, i):
        block = ((hi + HI - i // (2 * pieces)) % HI) * 2 + a
        return block, (i // pieces) % 2, i % pieces

    def place_o(q):
        return (row + R - q // (2 * pieces)) % R, (q // pieces) % 2, q % pieces

    def chunk(d, block, piece):
        return pl.ds(pl.multiple_of((d * R + block) * TB + piece * TC, TC), TC)

    def xs_copy(q, e):
        block, kk, piece = place_o(q)
        at = slopes.at[kk, chunk(dp, block, piece), :]
        return copy(at, at, xs_s.at[e - 1], xs_r.at[e - 1], dp=(dp + e) % D)

    def xs_whole(e):
        at = slopes.at[:, pl.ds(pl.multiple_of(dp * R * TB, R * TB), R * TB), :]
        return copy(at, at, xs_s.at[e - 1], xs_r.at[e - 1], dp=(dp + e) % D)

    def vt_copy(o):
        return copy(vt_all.at[row], vt_all.at[row], vt_s.at[o - 1], vt_r.at[o - 1],
                    row=(row + o) % R)

    def gl_copy(x, a):
        c, d = plane[x]
        return copy(gl.at[dp, a], gl.at[dp, a], gl_s.at[x], gl_r.at[a, x],
                    col=(col + c) % C, dp=(dp + d) % D)

    def vo_copy(x):
        r, d = group[x]
        return copy(vo_all.at[dp, row], vo_all.at[dp, row], vo_s.at[x], vo_r.at[x],
                    row=(row + r) % R, dp=(dp + d) % D)

    lane = lax.broadcasted_iota(jnp.int32, (TC, 128), 1)

    def note(store, block, kk, piece, gate, head):
        value = jnp.sum(gate * head, axis=1, keepdims=True)
        at = pl.ds(pl.multiple_of(piece * TC, TC), TC)
        store[at, :] += jnp.where(lane == kk * R + block, value, 0.0)

    def finish_t(a, i, pre):
        block, kk, piece = place_t(a, i)
        note(vals_t, block, kk, piece, pre * jax.nn.sigmoid(pre), thead[pl.ds(kk, 1), :])

    def finish_o(q, pre):
        block, kk, piece = place_o(q)
        sigma = jax.nn.sigmoid(pre)
        gate = pre * sigma
        head = chead[pl.ds(kk, 1), :]
        slopes[kk, chunk(dp, block, piece), :] = (
            head * (sigma * (1.0 + pre * (1.0 - sigma)))).astype(bf16)
        for e in range(1, D):
            xs_copy(q, e).start()
        hidden[kk, chunk(0, block, piece), :] = gate.astype(bf16)
        note(vals_o, block, kk, piece, gate, head)

    def settle(a, i):
        @pl.when(i == nt)
        def _():
            vt_all[row] = vals_t[...].T[:2 * R]
            for o in range(1, R):
                vt_copy(o).start()

        @pl.when(i == nt + 2 * pieces - 1)
        def _():
            for o in range(1, R):
                vt_copy(o).wait_recv()
            total = vt_all[0]
            for r in range(1, R):
                total = total + vt_all[r]
            reward = jnp.concatenate([rd_all[b, 0:1] for b in range(R)], axis=0)
            discount = jnp.concatenate([rd_all[b, 1:2] for b in range(R)], axis=0)
            goal = reward + discount * jnp.minimum(total[:R], total[R:])
            mine = lax.broadcasted_iota(jnp.int32, (R, TB), 0) % 2 == a
            goal = jnp.where(mine, goal, 0.0)
            gl[dp, a] = jnp.concatenate([goal, goal], axis=0)
            for x in range(len(plane)):
                gl_copy(x, a).start()

    def later(a, far):
        return 2 * far > C - 1 if a == 0 else 2 * far >= C - 1

    steps = n + lead + skew * (C - 1)

    def aside(s):
        @pl.when(s == 1)
        def _():
            for x in range(11, 16):
                loads[x].wait()
            for k in range(2):
                a16[k] = cact[k].astype(bf16)
                w16[k] = cin[k].astype(bf16)

        @pl.when(s == nt)
        def _():
            for o in range(1, R):
                rd_copy(o).wait_recv()

        @pl.when(s == nt + 2)
        def _():
            for e in range(1, D):
                ox_copy(e).wait_recv()
                for o in range(1, R):
                    oo_copy(e, o).start()

        @pl.when(s == nt + 1)
        def _():
            lift[...] = jnp.dot(a16[0], w16[0], preferred_element_type=f32).astype(bf16)

        for e in range(1, D):
            for o in range(R):
                @pl.when(s == nt + no // 2 + (e - 1) * R + o)
                def _():
                    if o > 0:
                        oo_copy(e, o).wait_recv()
                    embed_on((dp + D - e) % D, (row + R - o) % R)

    def step(s, carry):
        at = []
        for a in range(2):
            far = col if a == 0 else C - 1 - col
            i = s - skew * far - jnp.where(far > 0, lead, 0)
            at.append((a, far, i, (i >= 0) & (i < n)))

        for a, far, i, live in at:
            @pl.when(live)
            def _():
                early = i < nt
                q = i - nt
                tb, tk, tp = place_t(a, i)
                ob, ok, op = place_o(jnp.maximum(q, 0))
                kk = jnp.where(early, tk, ok)
                start = (jnp.where(early, D * R + tb, dp * R + ob) * TB
                         + jnp.where(early, tp, op) * TC)

                @pl.when(early)
                def _():
                    prepare_tg(a, i)

                @pl.when((q >= 0) & jnp.logical_not(later(a, far)))
                def _():
                    prepare_on(q)
                mine[a] = jnp.dot(emb[kk, pl.ds(pl.multiple_of(start, TC), TC), :],
                                  w16[jnp.where(early, 2, 0) + kk],
                                  preferred_element_type=f32)

        for a, far, i, live in at:
            @pl.when(live & (far == 0))
            def _():
                sums_out[a, i] = mine[a].astype(bf16)
                sm_copy(a, i).start()

        for a, far, i, live in at:
            @pl.when(live & (far > 0) & (far < C - 1))
            def _():
                sm_copy(a, i).wait_recv()
                total = mine[a] + sums_in[a, i].astype(f32)
                sums_out[a, i] = total.astype(bf16)
                sm_copy(a, i).start()
                mine[a] = total

            @pl.when(live & (far == C - 1))
            def _():
                sm_copy(a, i).wait_recv()
                mine[a] += sums_in[a, i].astype(f32)

        for a, far, i, live in at:
            @pl.when(live & (i < nt))
            def _():
                @pl.when(far == C - 1)
                def _():
                    finish_t(a, i, mine[a])
                forward_tg(a, i)

            @pl.when(live & (i >= nt) & later(a, far))
            def _():
                @pl.when(far < C - 1)
                def _():
                    mine[a] += sums_in[1 - a, i].astype(f32)
                finish_o(i - nt, mine[a])

            @pl.when(far == C - 1)
            def _():
                settle(a, i)
        aside(s)
        return carry

    lax.fori_loop(0, steps, step, 0)

    vo_all[dp, row] = vals_o[...].T[:2 * R]
    for x in range(len(group)):
        vo_copy(x).start()

    def pu_copy(o):
        return copy(pu_out.at[o - 1], pu_in.at[o - 1], pu_s.at[o - 1], pu_r.at[o - 1],
                    row=(row + o) % R)

    def pz_copy(c):
        return copy(pz_all.at[col], pz_all.at[col], pz_s.at[c - 1], pz_r.at[c - 1],
                    col=(col + c) % C)

    last = (((1,), (1,)), ((), ()))
    first = (((0,), (0,)), ((), ()))
    for o in list(range(1, R)) + [0]:
        got = lax.dot_general(slopes[0, rows_of(dp, (row + o) % R), :], lift[...], last,
                              preferred_element_type=f32)
        if o == 0:
            push_out[...] = got
        else:
            pu_out[o - 1] = got.astype(bf16)
            pu_copy(o).start()

    for a in range(2):
        end = C - 1 if a == 0 else 0
        for x, (c, d) in enumerate(plane):
            @pl.when((col + C - c) % C == end)
            def _():
                gl_copy(x, a).wait_recv()

    for e in range(1, D):
        xs_whole(e).wait_recv()
    for x in range(len(group)):
        vo_copy(x).wait_recv()

    epad[...] = jnp.zeros_like(epad)
    for d in range(D):
        value = vo_all[d, 0]
        for r in range(1, R):
            value = value + vo_all[d, r]
        err = value - (gl[d, 0] + gl[d, 1])
        err_own[d] = err
        epad[:2 * R, :] = 2.0 * err
        columns[d] = epad[...].T

    F2 = F // 2

    def ga_copy(k):
        return copy(ga_out.at[k, 1 - lo], ga_in.at[k], ga_s.at[k], ga_r.at[k], row=partner)

    def gb_copy(k, o):
        return copy(gb_all.at[k, hi], gb_all.at[k, hi], gb_s.at[k, o - 1], gb_r.at[k, o - 1],
                    row=((hi + o) % HI) * 2 + lo)

    def gc_copy(k):
        return copy(gc_all.at[k, lo], gc_all.at[k, lo], gc_s.at[k], gc_r.at[k], row=partner)

    chief = 1 % C

    def er_copy(c):
        return copy(err_top, err_top, er_s.at[c - 1], er_r.at[c - 1], col=(col + c) % C)

    def gh_copy(x):
        c, d = plane[x]
        return copy(gh.at[dp], gh.at[dp], gh_s.at[x], gh_r.at[x],
                    col=(col + c) % C, dp=(dp + d) % D)

    slot = lax.broadcasted_iota(jnp.int32, (2 * R, H), 0)

    @pl.when(col == chief)
    def _():
        err_top[...] = err_own[dp]
        for c in range(1, C):
            er_copy(c).start()
        twice = (2.0 * err_own[dp]).astype(bf16)
        total = jnp.zeros((2 * R, H), f32)
        for k in range(2):
            for b in range(R):
                got = jnp.dot(twice, hidden[k, b * TB:(b + 1) * TB, :],
                              preferred_element_type=f32)
                total = total + jnp.where(slot == k * R + b, got, 0.0)
        gh[dp] = total
        for x in range(len(plane)):
            gh_copy(x).start()

    for k in range(2):
        moved = jnp.zeros((A, H), f32)
        for d in range(D):
            for b in range(R):
                scaled[b * TB:(b + 1) * TB, :] = (
                    columns[d, :, k * R + b:k * R + b + 1] * on_all[d, b][:, F:].astype(f32)
                ).astype(bf16)
            moved = moved + lax.dot_general(
                scaled[...], slopes[k, d * R * TB:(d + 1) * R * TB, :], first,
                preferred_element_type=f32)
        term = lax.dot_general(moved.astype(bf16), w16[k], last, preferred_element_type=f32)

        for p in range(2):
            ga_own[k, p] = term[:, p * F2:(p + 1) * F2]
            ga_out[k, p] = term[:, p * F2:(p + 1) * F2].astype(bf16)
        ga_copy(k).start()

    for k in range(2):
        ga_copy(k).wait_recv()
        gb_all[k, hi] = (ga_own[k, lo] + ga_in[k].astype(f32)).astype(bf16)
        for o in range(1, HI):
            gb_copy(k, o).start()

    for o in range(1, R):
        pu_copy(o).wait_recv()
        push_out[...] += pu_in[o - 1].astype(f32)
    pz_all[col] = push_out[...].astype(bf16)
    for c in range(1, C):
        pz_copy(c).start()

    def blend(fresh, target):
        return blend_rate * fresh + (1.0 - blend_rate) * target

    def grad_in(k):
        def scale(d):
            for b in range(R):
                at = pl.ds(pl.multiple_of((d * R + b) * TB, TB), TB)
                delta[b * TB:(b + 1) * TB, :] = (
                    columns[d, :, k * R + b:k * R + b + 1] * slopes[k, at, :].astype(f32)
                ).astype(bf16)
            at = pl.ds(pl.multiple_of(d * R * TB, R * TB), R * TB)
            return lax.dot_general(emb[k, at, :], delta[...], first, preferred_element_type=f32)

        def add(d, carry):
            new_in[k] += scale(d)
            return carry
        new_in[k] = scale(0)
        lax.fori_loop(1, D, add, 0)
        fresh = cin[k] - matrix_rate * new_in[k]
        new_in[k] = fresh
        new_tin[k] = blend(fresh, tin[k])

    grad_in(0)
    grad_in(1)

    for k in range(2):
        for o in range(1, HI):
            gb_copy(k, o).wait_recv()
        piece = gb_all[k, 0].astype(f32)
        for h in range(1, HI):
            piece = piece + gb_all[k, h].astype(f32)
        gc_all[k, lo] = piece.astype(bf16)
        gc_copy(k).start()

    for c in range(1, C):
        pz_copy(c).wait_recv()
    push = pz_all[0].astype(f32)
    for c in range(1, C):
        push = push + pz_all[c].astype(f32)
    epad[0:1, :] = flags[...].astype(f32)
    flag_column[...] = epad[...].T[:, 0:1]
    push_out[...] = push * flag_column[...]

    for c in range(1, C):
        @pl.when(col == (chief + c) % C)
        def _():
            er_copy(c).wait_recv()
    for k in range(2):
        errs_out[k:k + 1, :] = err_top[pl.ds(k * R + row, 1), :]

    for x, (c, d) in enumerate(plane):
        @pl.when(col == (chief + c) % C)
        def _():
            gh_copy(x).wait_recv()
    whole = gh[0]
    for d in range(1, D):
        whole = whole + gh[d]
    for k in range(2):
        grad = jnp.sum(whole[k * R:(k + 1) * R], axis=0, keepdims=True)
        fresh = chead[k:k + 1, :] - head_rate * grad
        new_head[k:k + 1, :] = fresh
        new_thead[k:k + 1, :] = blend(fresh, thead[k:k + 1, :])

    for k in range(2):
        gc_copy(k).wait_recv()
        for p in range(2):
            part = slice(p * F2, (p + 1) * F2)
            fresh = cact[k, :, part] - matrix_rate * gc_all[k, p].astype(f32)
            new_act[k, :, part] = fresh
            new_tact[k, :, part] = blend(fresh, tact[k, :, part])

    for o in range(HI):
        tg_copy(o).wait_send()
        if o > 0:
            ftg_copy(o, row).wait_send()
    for o in range(1, R):
        on_copy(o).wait_send()
        rd_copy(o).wait_send()
        pu_copy(o).wait_send()
        for e in range(1, D):
            oo_copy(e, o).wait_send()
    for e in range(1, D):
        ox_copy(e).wait_send()
    for a in range(2):
        far = col if a == 0 else C - 1 - col

        @pl.when(far < C - 1)
        def _():
            sm_sent(a).wait_send()

        @pl.when(far == C - 1)
        def _():
            for o in range(1, R):
                vt_copy(o).wait_send()
            for x in range(len(plane)):
                gl_copy(x, a).wait_send()

    for e in range(1, D):
        xs_whole(e).wait_send()
    for x in range(len(group)):
        vo_copy(x).wait_send()
    for c in range(1, C):
        pz_copy(c).wait_send()

    @pl.when(col == chief)
    def _():
        for c in range(1, C):
            er_copy(c).wait_send()
        for x in range(len(plane)):
            gh_copy(x).wait_send()
    for k in range(2):
        ga_copy(k).wait_send()
        gc_copy(k).wait_send()
        for o in range(1, HI):
            gb_copy(k, o).wait_send()


def put_out(*refs):
    count = len(refs) // 2
    copies = [pltpu.make_async_copy(refs[x], refs[count + x], refs[-1].at[x])
              for x in range(count)]
    for one in copies:
        one.start()
    for one in copies:
        one.wait()


def on_device(dims, observed, next_observed, actions, next_mean, policy_noise, rewards, discounts,
              actor_flags, critic_in, critic_act, critic_head, target_in, target_act, target_head):
    R, C, D, TB, F, H, A = dims
    HI, TC = R // 2, TB // pieces
    nt, no = 2 * HI * pieces, 2 * R * pieces
    planes, groups = C * D - 1, R * D - 1
    dma = lambda *shape: pltpu.SemaphoreType.DMA(shape)
    vmem = pltpu.VMEM
    scratch = [
        vmem((TB, A), bf16), vmem((TB, A), f32), vmem((1, TB), bf16), vmem((1, TB), bf16),
        vmem((1, TB), jnp.int32), vmem((2, F, H), f32), vmem((2, A, F), f32), vmem((2, H), f32),
        vmem((2, F, H), f32), vmem((2, A, F), f32), vmem((2, H), f32),
        vmem((TB, F + A), bf16), vmem((TB, F + A), bf16), vmem((TB, 1), f32),
        vmem((4, F, H), bf16), vmem((4, A, F), bf16),
        vmem((D, R, TB, F + A), bf16), vmem((R, TB, F + A), bf16),
        vmem((2, (D + 1) * R * TB, F), bf16),
        vmem((2, D * R * TB, H), bf16), vmem((R * TB, H), bf16), vmem((A, H), bf16),
        vmem((2, nt + no, TC, H), bf16), vmem((2, nt + no, TC, H), bf16), vmem((2, TC, H), f32),
        vmem((2, R * TB, H), bf16), vmem((TB, 128), f32), vmem((TB, 128), f32),
        vmem((8, TB), f32), vmem((R, 8, TB), f32), vmem((R, 2 * R, TB), f32),
        vmem((D, R, 2 * R, TB), f32), vmem((D, 2, 2 * R, TB), f32),
        vmem((D, 2 * R, TB), f32), vmem((2 * R, TB), f32), vmem((D, 2 * R, H), f32),
        vmem((128, TB), f32), vmem((D, TB, 128), f32), vmem((R * TB, A), bf16),
        vmem((2, 2, A, F // 2), f32), vmem((2, 2, A, F // 2), bf16), vmem((2, A, F // 2), bf16),
        vmem((2, HI, A, F // 2), bf16), vmem((2, 2, A, F // 2), bf16),
        vmem((R - 1, TB, A), bf16), vmem((R - 1, TB, A), bf16), vmem((C, TB, A), bf16),
        dma(16),
        dma(R - 1), dma(R - 1), dma(HI), dma(HI), dma(HI), dma(HI),
        dma(D - 1), dma(D - 1), dma(D - 1, R - 1), dma(D - 1, R - 1), dma(R - 1), dma(R - 1),
        dma(2), dma(2, nt + no), dma(D - 1), dma(D - 1),
        dma(R - 1), dma(R - 1), dma(groups), dma(groups), dma(planes), dma(2, planes),
        dma(C - 1), dma(C - 1), dma(planes), dma(planes),
        dma(2), dma(2), dma(2, HI - 1), dma(2, HI - 1), dma(2), dma(2),
        dma(R - 1), dma(R - 1), dma(C - 1), dma(C - 1),
    ]
    spec = pl.BlockSpec(memory_space=vmem)
    results = (((2, F, H), f32), ((2, A, F), f32), ((2, H), f32), ((2, F, H), f32),
               ((2, A, F), f32), ((2, H), f32), ((2, TB), f32), ((TB, A), f32))
    kept = pl.pallas_call(
        functools.partial(kernel, dims),
        out_shape=tuple(vmem(shape, kind) for shape, kind in results),
        in_specs=[pl.BlockSpec(memory_space=pltpu.HBM)] * 14,
        out_specs=(spec,) * len(results),
        scratch_shapes=scratch,
        compiler_params=pltpu.CompilerParams(
            collective_id=0, has_side_effects=True, vmem_limit_bytes=57 * 2 ** 20),
    )(*[pltpu.with_memory_space_constraint(one, pltpu.HBM) for one in (
        observed, next_observed, actions, next_mean, policy_noise, rewards[None, :],
        discounts[None, :], actor_flags[None, :], critic_in, critic_act, critic_head, target_in,
        target_act, target_head)])
    return pl.pallas_call(
        put_out,
        out_shape=tuple(jax.ShapeDtypeStruct(shape, kind) for shape, kind in results),
        in_specs=[spec] * len(results),
        out_specs=(pl.BlockSpec(memory_space=pl.ANY),) * len(results),
        scratch_shapes=[dma(len(results))],
        compiler_params=pltpu.CompilerParams(vmem_limit_bytes=12 * 2 ** 20),
    )(*[pltpu.with_memory_space_constraint(one, vmem) for one in kept])


def solution(mesh):
    def run(*args):
        R, C, D = mesh.shape["row"], mesh.shape["col"], mesh.shape["dp"]
        tokens, features = args[0].shape
        dims = (R, C, D, tokens // (R * D), features // C, args[8].shape[2] // R,
                args[2].shape[1])
        return sharded(dims)(*args)

    def sharded(dims):
        return jax.shard_map(
            functools.partial(on_device, dims),
            mesh=mesh,
            in_specs=(
                P(("row", "dp"), "col"),
                P(("row", "dp"), "col"),
                P(("row", "dp"), None),
                P(("row", "dp"), None),
                P(("row", "dp"), None),
                P(("row", "dp")),
                P(("row", "dp")),
                P(("row", "dp")),
                P(None, "col", "row"),
                P(None, None, "col"),
                P(None, "row"),
                P(None, "col", "row"),
                P(None, None, "col"),
                P(None, "row"),
            ),
            out_specs=(
                P(None, "col", "row"),
                P(None, None, "col"),
                P(None, "row"),
                P(None, "col", "row"),
                P(None, None, "col"),
                P(None, "row"),
                P(None, ("row", "dp")),
                P(("row", "dp"), None),
            ),
            check_vma=False,
        )

    return run
```

```python
import functools

import jax
import jax.numpy as jnp
from jax import lax
from jax.experimental import pallas as pl
from jax.experimental.pallas import tpu as pltpu
from jax.sharding import PartitionSpec as P

noise_clip = 0.5
matrix_rate = 0.004
head_rate = 0.0001
blend_rate = 0.005

f32 = jnp.float32
bf16 = jnp.bfloat16
pace = 5
lead = 2
pieces = 2


def kernel(dims, observed_at, next_observed_at, actions_at, next_mean_at, noise_at, rewards_at,
           discounts_at, flags_at, cin_at, cact_at, chead_at, tin_at, tact_at, thead_at,
           new_in, new_act, new_head, new_tin, new_tact, new_thead, errs_out, push_out,
           next_mean, noise, rewards, discounts, flags, cin, cact, chead, tin, tact, thead,
           on_own, tg_own, flag_column, w16, a16, on_all, tg_all, emb, slopes, turned, lift,
           sums_out, sums_in, mine, hidden, vals_t, vals_o, rd_own, rd_all, vt_all, vo_all, gl,
           err_own, err_top, gh, epad, columns,
           ga_own, ga_out, ga_in, gb_all, gc_all, pu_out, pu_in, pz_all,
           load_s, on_s, on_r, tg_s, tg_r, ftg_s, ftg_r, ox_s, ox_r, oo_s, oo_r, rd_s, rd_r,
           sm_s, sm_r, xs_s, xs_r, vt_s, vt_r, vo_s, vo_r, gl_s, gl_r, er_s, er_r,
           gh_s, gh_r, ga_s, ga_r, gb_s, gb_r, gc_s, gc_r, pu_s, pu_r, pz_s, pz_r):
    R, C, D, TB, F, H, A = dims
    HI = R // 2
    TC = TB // pieces
    row, col, dp = lax.axis_index("row"), lax.axis_index("col"), lax.axis_index("dp")
    hi, lo = row // 2, row % 2
    nt = 2 * HI * pieces
    no = 2 * R * pieces
    n = nt + no
    partner = hi * 2 + (1 - lo)

    def copy(src, dst, ssem, rsem, **where):
        return pltpu.make_async_remote_copy(
            src_ref=src, dst_ref=dst, send_sem=ssem, recv_sem=rsem,
            device_id=where, device_id_type=pl.DeviceIdType.MESH)

    pairs = [(next_observed_at, tg_own.at[:, :F]), (next_mean_at, next_mean), (noise_at, noise),
             (tact_at, tact), (tin_at.at[0], tin.at[0]), (tin_at.at[1], tin.at[1]),
             (thead_at, thead), (observed_at, on_own.at[:, :F]), (actions_at, on_own.at[:, F:]),
             (rewards_at, rewards), (discounts_at, discounts), (flags_at, flags),
             (cact_at, cact), (cin_at.at[0], cin.at[0]), (cin_at.at[1], cin.at[1]),
             (chead_at, chead)]
    loads = [pltpu.make_async_copy(src, dst, load_s.at[x]) for x, (src, dst) in enumerate(pairs)]
    for load in loads:
        load.start()

    plane = [(c, d) for d in range(D) for c in range(C) if c or d]
    group = [(r, d) for d in range(D) for r in range(R) if r or d]
    others = [(r, 0, d) for r, d in group] + [(0, c, d) for c, d in plane if c]
    barrier = pltpu.get_barrier_semaphore()
    for r, c, d in others:
        pl.semaphore_signal(barrier, inc=1,
                            device_id={"row": (row + r) % R, "col": (col + c) % C,
                                       "dp": (dp + d) % D},
                            device_id_type=pl.DeviceIdType.MESH)

    vals_t[...] = jnp.zeros_like(vals_t)
    vals_o[...] = jnp.zeros_like(vals_o)
    for x in range(3):
        loads[x].wait()
    tg_own[:, F:] = jnp.clip(
        next_mean[...].astype(f32) + jnp.clip(noise[...], -noise_clip, noise_clip), -1.0, 1.0
    ).astype(bf16)
    pl.semaphore_wait(barrier, len(others))

    def tg_copy(o):
        to = partner if o == 0 else ((hi + o) % HI) * 2 + lo
        return copy(tg_own, tg_all.at[row], tg_s.at[o], tg_r.at[o], row=to)

    def ftg_copy(o, block):
        return copy(tg_all.at[block], tg_all.at[block], ftg_s.at[o], ftg_r.at[o], row=partner)

    def on_copy(o):
        return copy(on_own, on_all.at[dp, row], on_s.at[o - 1], on_r.at[o - 1],
                    row=(row + o) % R)

    def ox_copy(e):
        return copy(on_own, on_all.at[dp, row], ox_s.at[e - 1], ox_r.at[e - 1], dp=(dp + e) % D)

    def oo_copy(e, o):
        at = on_all.at[(dp + D - e) % D, row]
        return copy(at, at, oo_s.at[e - 1, o - 1], oo_r.at[e - 1, o - 1], row=(row + o) % R)

    def rd_copy(o):
        return copy(rd_own, rd_all.at[row], rd_s.at[o - 1], rd_r.at[o - 1], row=(row + o) % R)

    for o in range(HI):
        tg_copy(o).start()
    tg_all[row] = tg_own[...]
    for x in range(9, 11):
        loads[x].wait()
    rd_own[...] = jnp.zeros_like(rd_own)
    rd_own[0:1, :] = rewards[...].astype(f32)
    rd_own[1:2, :] = discounts[...].astype(f32)
    for o in range(1, R):
        rd_copy(o).start()
    rd_all[row] = rd_own[...]
    for x in range(3, 7):
        loads[x].wait()
    for k in range(2):
        a16[2 + k] = tact[k].astype(bf16)
        w16[2 + k] = tin[k].astype(bf16)
    for x in (7, 8):
        loads[x].wait()
    for e in range(1, D):
        ox_copy(e).start()
    for o in range(1, R):
        on_copy(o).start()
    on_all[dp, row] = on_own[...]

    def rows_of(d, block):
        return pl.ds(pl.multiple_of((d * R + block) * TB, TB), TB)

    def embed_on(d, block):
        x = on_all[d, block]
        turned[:, rows_of(d, block)] = x[:, F:].T
        for k in range(2):
            mixed = jnp.dot(x[:, F:], a16[k], preferred_element_type=f32)
            emb[k, rows_of(d, block), :] = (x[:, :F].astype(f32) + mixed).astype(bf16)

    def embed_tg(block):
        x = tg_all[block]
        for k in range(2):
            mixed = jnp.dot(x[:, F:], a16[2 + k], preferred_element_type=f32)
            emb[k, rows_of(D, block), :] = (x[:, :F].astype(f32) + mixed).astype(bf16)

    def prepare_tg(a, i):
        for o in range(HI):
            block = ((hi + HI - o) % HI) * 2 + a

            @pl.when(i == 2 * pieces * o)
            def _():
                @pl.when(lo != a)
                def _():
                    if o > 0:
                        ftg_copy(o, block).wait_recv()
                    else:
                        tg_copy(0).wait_recv()
                embed_tg(block)

    def forward_tg(a, i, far):
        for o in range(1, HI):
            @pl.when((i == 2 * pieces * o - jnp.where(far == 0, 1, pieces + 1)) & (lo == a))
            def _():
                tg_copy(o).wait_recv()
                ftg_copy(o, ((hi + HI - o) % HI) * 2 + a).start()

    def prepare_on(q):
        for o in range(R):
            @pl.when(q == 2 * pieces * o)
            def _():
                if o > 0:
                    on_copy(o).wait_recv()
                embed_on(dp, (row + R - o) % R)

    def along(a):
        return jnp.where(a == 0, col + 1, col + C - 1) % C

    def sm_copy(a, i):
        return copy(sums_out.at[a, i], sums_in.at[a, i], sm_s.at[a], sm_r.at[a, i], col=along(a))

    def sm_sent(a):
        return copy(sums_out.at[a], sums_in.at[a], sm_s.at[a], sm_r.at[a, 0], col=along(a))

    def place_t(a, i):
        block = ((hi + HI - i // (2 * pieces)) % HI) * 2 + a
        return block, (i // pieces) % 2, i % pieces

    def place_o(q):
        return (row + R - q // (2 * pieces)) % R, (q // pieces) % 2, q % pieces

    def chunk(d, block, piece):
        return pl.ds(pl.multiple_of((d * R + block) * TB + piece * TC, TC), TC)

    def xs_copy(q, e):
        block, kk, piece = place_o(q)
        at = slopes.at[kk, chunk(dp, block, piece), :]
        return copy(at, at, xs_s.at[kk, e - 1], xs_r.at[kk, e - 1], dp=(dp + e) % D)

    def xs_whole(k, e):
        at = slopes.at[k, pl.ds(pl.multiple_of(dp * R * TB, R * TB), R * TB), :]
        return copy(at, at, xs_s.at[k, e - 1], xs_r.at[k, e - 1], dp=(dp + e) % D)

    def vt_copy(o):
        return copy(vt_all.at[row], vt_all.at[row], vt_s.at[o - 1], vt_r.at[o - 1],
                    row=(row + o) % R)

    def gl_copy(x, a):
        c, d = plane[x]
        return copy(gl.at[dp, a], gl.at[dp, a], gl_s.at[x], gl_r.at[a, x],
                    col=(col + c) % C, dp=(dp + d) % D)

    def vo_copy(x):
        r, d = group[x]
        return copy(vo_all.at[dp, row], vo_all.at[dp, row], vo_s.at[x], vo_r.at[x],
                    row=(row + r) % R, dp=(dp + d) % D)

    lane = lax.broadcasted_iota(jnp.int32, (TC, 128), 1)

    def note(store, block, kk, piece, gate, head):
        value = jnp.sum(gate * head, axis=1, keepdims=True)
        at = pl.ds(pl.multiple_of(piece * TC, TC), TC)
        store[at, :] += jnp.where(lane == kk * R + block, value, 0.0)

    def finish_t(a, i, pre):
        block, kk, piece = place_t(a, i)
        note(vals_t, block, kk, piece, pre * jax.nn.sigmoid(pre), thead[pl.ds(kk, 1), :])

    def finish_o(q, pre):
        block, kk, piece = place_o(q)
        sigma = jax.nn.sigmoid(pre)
        gate = pre * sigma
        head = chead[pl.ds(kk, 1), :]
        slopes[kk, chunk(dp, block, piece), :] = (
            head * (sigma * (1.0 + pre * (1.0 - sigma)))).astype(bf16)
        hidden[kk, chunk(0, block, piece), :] = gate.astype(bf16)
        note(vals_o, block, kk, piece, gate, head)

        @pl.when(q == no - 1)
        def _():
            vo_all[dp, row] = vals_o[...].T[:2 * R]
            for x in range(len(group)):
                vo_copy(x).start()
        for e in range(1, D):
            xs_copy(q, e).start()

    def settle(a, i):
        @pl.when(i == nt)
        def _():
            vt_all[row] = vals_t[...].T[:2 * R]
            for o in range(1, R):
                vt_copy(o).start()

        @pl.when(i == nt + 2 * pieces - 1)
        def _():
            for o in range(1, R):
                vt_copy(o).wait_recv()
            total = vt_all[0]
            for r in range(1, R):
                total = total + vt_all[r]
            reward = jnp.concatenate([rd_all[b, 0:1] for b in range(R)], axis=0)
            discount = jnp.concatenate([rd_all[b, 1:2] for b in range(R)], axis=0)
            goal = reward + discount * jnp.minimum(total[:R], total[R:])
            mine = lax.broadcasted_iota(jnp.int32, (R, TB), 0) % 2 == a
            goal = jnp.where(mine, goal, 0.0)
            gl[dp, a] = jnp.concatenate([goal, goal], axis=0)
            for x in range(len(plane)):
                gl_copy(x, a).start()

    def later(a, far):
        return 2 * far + a > C - 1

    steps = n + lead + pace * (C - 1) // 2

    def aside(s):
        @pl.when(s == 1)
        def _():
            for x in range(11, 16):
                loads[x].wait()
            for k in range(2):
                a16[k] = cact[k].astype(bf16)
                w16[k] = cin[k].astype(bf16)

        @pl.when(s == nt)
        def _():
            for o in range(1, R):
                rd_copy(o).wait_recv()

        @pl.when(s == nt + 2)
        def _():
            for e in range(1, D):
                ox_copy(e).wait_recv()
                for o in range(1, R):
                    oo_copy(e, o).start()

        @pl.when(s == nt + 1)
        def _():
            lift[...] = jnp.dot(a16[0], w16[0], preferred_element_type=f32).astype(bf16)

        for e in range(1, D):
            for o in range(R):
                @pl.when(s == nt + no // 2 + (e - 1) * R + o)
                def _():
                    if o > 0:
                        oo_copy(e, o).wait_recv()
                    embed_on((dp + D - e) % D, (row + R - o) % R)

    def step(s, carry):
        at = []
        for j in range(2):
            a = (col + j) % 2
            far = jnp.where(a == 0, col, C - 1 - col)
            i = s - pace * far // 2 - jnp.where(far > 0, lead, 0)
            at.append((a, far, i, (i >= 0) & (i < n)))

        for a, far, i, live in at:
            @pl.when(live)
            def _():
                early = i < nt
                q = i - nt
                tb, tk, tp = place_t(a, i)
                ob, ok, op = place_o(jnp.maximum(q, 0))
                kk = jnp.where(early, tk, ok)
                start = (jnp.where(early, D * R + tb, dp * R + ob) * TB
                         + jnp.where(early, tp, op) * TC)

                @pl.when(early)
                def _():
                    prepare_tg(a, i)

                @pl.when((q >= 0) & jnp.logical_not(later(a, far)))
                def _():
                    prepare_on(q)
                mine[a] = jnp.dot(emb[kk, pl.ds(pl.multiple_of(start, TC), TC), :],
                                  w16[jnp.where(early, 2, 0) + kk],
                                  preferred_element_type=f32)

        for a, far, i, live in at:
            @pl.when(live & (far == 0))
            def _():
                sums_out[a, i] = mine[a].astype(bf16)
                sm_copy(a, i).start()

        for a, far, i, live in at:
            @pl.when(live & (far > 0) & (far < C - 1))
            def _():
                sm_copy(a, i).wait_recv()
                total = mine[a] + sums_in[a, i].astype(f32)
                sums_out[a, i] = total.astype(bf16)
                sm_copy(a, i).start()
                mine[a] = total

            @pl.when(live & (far == C - 1))
            def _():
                sm_copy(a, i).wait_recv()
                mine[a] += sums_in[a, i].astype(f32)

        for a, far, i, live in at:
            @pl.when(live & (i < nt))
            def _():
                @pl.when(far == C - 1)
                def _():
                    finish_t(a, i, mine[a])
                forward_tg(a, i, far)

            @pl.when(live & (i >= nt) & later(a, far))
            def _():
                @pl.when(far < C - 1)
                def _():
                    mine[a] += sums_in[1 - a, i].astype(f32)
                finish_o(i - nt, mine[a])

            @pl.when(far == C - 1)
            def _():
                settle(a, i)
        aside(s)
        return carry

    lax.fori_loop(0, steps, step, 0)

    def pu_copy(o):
        return copy(pu_out.at[o - 1], pu_in.at[o - 1], pu_s.at[o - 1], pu_r.at[o - 1],
                    row=(row + o) % R)

    def pz_copy(c):
        return copy(pz_all.at[col], pz_all.at[col], pz_s.at[c - 1], pz_r.at[c - 1],
                    col=(col + c) % C)

    last = (((1,), (1,)), ((), ()))
    first = (((0,), (0,)), ((), ()))
    for o in list(range(1, R)) + [0]:
        got = lax.dot_general(slopes[0, rows_of(dp, (row + o) % R), :], lift[...], last,
                              preferred_element_type=f32)
        if o == 0:
            push_out[...] = got
        else:
            pu_out[o - 1] = got.astype(bf16)
            pu_copy(o).start()

    for a in range(2):
        end = C - 1 if a == 0 else 0
        for x, (c, d) in enumerate(plane):
            @pl.when((col + C - c) % C == end)
            def _():
                gl_copy(x, a).wait_recv()

    for x in range(len(group)):
        vo_copy(x).wait_recv()

    epad[...] = jnp.zeros_like(epad)
    for d in range(D):
        value = vo_all[d, 0]
        for r in range(1, R):
            value = value + vo_all[d, r]
        err = value - (gl[d, 0] + gl[d, 1])
        err_own[d] = err
        epad[:2 * R, :] = 2.0 * err
        columns[d] = epad[...].T

    F2 = F // 2

    def ga_copy(k):
        return copy(ga_out.at[k, 1 - lo], ga_in.at[k], ga_s.at[k], ga_r.at[k], row=partner)

    def gb_copy(k, o):
        return copy(gb_all.at[k, hi], gb_all.at[k, hi], gb_s.at[k, o - 1], gb_r.at[k, o - 1],
                    row=((hi + o) % HI) * 2 + lo)

    def gc_copy(k):
        return copy(gc_all.at[k, lo], gc_all.at[k, lo], gc_s.at[k], gc_r.at[k], row=partner)

    chief = 1 % C

    def er_copy(c):
        return copy(err_top, err_top, er_s.at[c - 1], er_r.at[c - 1], col=(col + c) % C)

    def gh_copy(x):
        c, d = plane[x]
        return copy(gh.at[dp], gh.at[dp], gh_s.at[x], gh_r.at[x],
                    col=(col + c) % C, dp=(dp + d) % D)

    slot = lax.broadcasted_iota(jnp.int32, (2 * R, H), 0)

    @pl.when(col == chief)
    def _():
        err_top[...] = err_own[dp]
        for c in range(1, C):
            er_copy(c).start()
        twice = (2.0 * err_own[dp]).astype(bf16)
        total = jnp.zeros((2 * R, H), f32)
        for k in range(2):
            for b in range(R):
                got = jnp.dot(twice, hidden[k, b * TB:(b + 1) * TB, :],
                              preferred_element_type=f32)
                total = total + jnp.where(slot == k * R + b, got, 0.0)
        gh[dp] = total
        for x in range(len(plane)):
            gh_copy(x).start()

    for k in range(2):
        for e in range(1, D):
            xs_whole(k, e).wait()
        moved = jnp.zeros((A, H), f32)
        for d in range(D):
            for b in range(R):
                at = slice((d * R + b) * TB, (d * R + b + 1) * TB)
                slopes[k, at, :] = (columns[d, :, k * R + b:k * R + b + 1]
                                    * slopes[k, at, :].astype(f32)).astype(bf16)
            at = slice(d * R * TB, (d + 1) * R * TB)
            moved = moved + jnp.dot(turned[:, at], slopes[k, at, :],
                                    preferred_element_type=f32)
        term = lax.dot_general(moved.astype(bf16), w16[k], last, preferred_element_type=f32)

        for p in range(2):
            ga_own[k, p] = term[:, p * F2:(p + 1) * F2]
            ga_out[k, p] = term[:, p * F2:(p + 1) * F2].astype(bf16)
        ga_copy(k).start()

    for k in range(2):
        ga_copy(k).wait_recv()
        gb_all[k, hi] = (ga_own[k, lo] + ga_in[k].astype(f32)).astype(bf16)
        for o in range(1, HI):
            gb_copy(k, o).start()

    for o in range(1, R):
        pu_copy(o).wait_recv()
        push_out[...] += pu_in[o - 1].astype(f32)
    pz_all[col] = push_out[...].astype(bf16)
    for c in range(1, C):
        pz_copy(c).start()

    def blend(fresh, target):
        return blend_rate * fresh + (1.0 - blend_rate) * target

    def grad_in(k):
        def part(d):
            at = pl.ds(pl.multiple_of(d * R * TB, R * TB), R * TB)
            return lax.dot_general(emb[k, at, :], slopes[k, at, :], first,
                                   preferred_element_type=f32)

        def add(d, carry):
            new_in[k] += part(d)
            return carry
        new_in[k] = part(0)
        lax.fori_loop(1, D, add, 0)
        fresh = cin[k] - matrix_rate * new_in[k]
        new_in[k] = fresh
        new_tin[k] = blend(fresh, tin[k])

    grad_in(0)
    grad_in(1)

    for k in range(2):
        for o in range(1, HI):
            gb_copy(k, o).wait_recv()
        piece = gb_all[k, 0].astype(f32)
        for h in range(1, HI):
            piece = piece + gb_all[k, h].astype(f32)
        gc_all[k, lo] = piece.astype(bf16)
        gc_copy(k).start()

    for c in range(1, C):
        pz_copy(c).wait_recv()
    push = pz_all[0].astype(f32)
    for c in range(1, C):
        push = push + pz_all[c].astype(f32)
    epad[0:1, :] = flags[...].astype(f32)
    flag_column[...] = epad[...].T[:, 0:1]
    push_out[...] = push * flag_column[...]

    for c in range(1, C):
        @pl.when(col == (chief + c) % C)
        def _():
            er_copy(c).wait_recv()
    for k in range(2):
        errs_out[k:k + 1, :] = err_top[pl.ds(k * R + row, 1), :]

    for x, (c, d) in enumerate(plane):
        @pl.when(col == (chief + c) % C)
        def _():
            gh_copy(x).wait_recv()
    whole = gh[0]
    for d in range(1, D):
        whole = whole + gh[d]
    for k in range(2):
        grad = jnp.sum(whole[k * R:(k + 1) * R], axis=0, keepdims=True)
        fresh = chead[k:k + 1, :] - head_rate * grad
        new_head[k:k + 1, :] = fresh
        new_thead[k:k + 1, :] = blend(fresh, thead[k:k + 1, :])

    for k in range(2):
        gc_copy(k).wait_recv()
        for p in range(2):
            part = slice(p * F2, (p + 1) * F2)
            fresh = cact[k, :, part] - matrix_rate * gc_all[k, p].astype(f32)
            new_act[k, :, part] = fresh
            new_tact[k, :, part] = blend(fresh, tact[k, :, part])

    for o in range(HI):
        tg_copy(o).wait_send()
        if o > 0:
            ftg_copy(o, row).wait_send()
    for o in range(1, R):
        on_copy(o).wait_send()
        rd_copy(o).wait_send()
        pu_copy(o).wait_send()
        for e in range(1, D):
            oo_copy(e, o).wait_send()
    for e in range(1, D):
        ox_copy(e).wait_send()
    for a in range(2):
        far = col if a == 0 else C - 1 - col

        @pl.when(far < C - 1)
        def _():
            sm_sent(a).wait_send()

        @pl.when(far == C - 1)
        def _():
            for o in range(1, R):
                vt_copy(o).wait_send()
            for x in range(len(plane)):
                gl_copy(x, a).wait_send()

    for x in range(len(group)):
        vo_copy(x).wait_send()
    for c in range(1, C):
        pz_copy(c).wait_send()

    @pl.when(col == chief)
    def _():
        for c in range(1, C):
            er_copy(c).wait_send()
        for x in range(len(plane)):
            gh_copy(x).wait_send()
    for k in range(2):
        ga_copy(k).wait_send()
        gc_copy(k).wait_send()
        for o in range(1, HI):
            gb_copy(k, o).wait_send()


def put_out(*refs):
    count = len(refs) // 2
    copies = [pltpu.make_async_copy(refs[x], refs[count + x], refs[-1].at[x])
              for x in range(count)]
    for one in copies:
        one.start()
    for one in copies:
        one.wait()


def on_device(dims, observed, next_observed, actions, next_mean, policy_noise, rewards, discounts,
              actor_flags, critic_in, critic_act, critic_head, target_in, target_act, target_head):
    R, C, D, TB, F, H, A = dims
    HI, TC = R // 2, TB // pieces
    nt, no = 2 * HI * pieces, 2 * R * pieces
    planes, groups = C * D - 1, R * D - 1
    dma = lambda *shape: pltpu.SemaphoreType.DMA(shape)
    vmem = pltpu.VMEM
    scratch = [
        vmem((TB, A), bf16), vmem((TB, A), f32), vmem((1, TB), bf16), vmem((1, TB), bf16),
        vmem((1, TB), jnp.int32), vmem((2, F, H), f32), vmem((2, A, F), f32), vmem((2, H), f32),
        vmem((2, F, H), f32), vmem((2, A, F), f32), vmem((2, H), f32),
        vmem((TB, F + A), bf16), vmem((TB, F + A), bf16), vmem((TB, 1), f32),
        vmem((4, F, H), bf16), vmem((4, A, F), bf16),
        vmem((D, R, TB, F + A), bf16), vmem((R, TB, F + A), bf16),
        vmem((2, (D + 1) * R * TB, F), bf16),
        vmem((2, D * R * TB, H), bf16), vmem((A, D * R * TB), bf16), vmem((A, H), bf16),
        vmem((2, nt + no, TC, H), bf16), vmem((2, nt + no, TC, H), bf16), vmem((2, TC, H), f32),
        vmem((2, R * TB, H), bf16), vmem((TB, 128), f32), vmem((TB, 128), f32),
        vmem((8, TB), f32), vmem((R, 8, TB), f32), vmem((R, 2 * R, TB), f32),
        vmem((D, R, 2 * R, TB), f32), vmem((D, 2, 2 * R, TB), f32),
        vmem((D, 2 * R, TB), f32), vmem((2 * R, TB), f32), vmem((D, 2 * R, H), f32),
        vmem((128, TB), f32), vmem((D, TB, 128), f32),
        vmem((2, 2, A, F // 2), f32), vmem((2, 2, A, F // 2), bf16), vmem((2, A, F // 2), bf16),
        vmem((2, HI, A, F // 2), bf16), vmem((2, 2, A, F // 2), bf16),
        vmem((R - 1, TB, A), bf16), vmem((R - 1, TB, A), bf16), vmem((C, TB, A), bf16),
        dma(16),
        dma(R - 1), dma(R - 1), dma(HI), dma(HI), dma(HI), dma(HI),
        dma(D - 1), dma(D - 1), dma(D - 1, R - 1), dma(D - 1, R - 1), dma(R - 1), dma(R - 1),
        dma(2), dma(2, nt + no), dma(2, D - 1), dma(2, D - 1),
        dma(R - 1), dma(R - 1), dma(groups), dma(groups), dma(planes), dma(2, planes),
        dma(C - 1), dma(C - 1), dma(planes), dma(planes),
        dma(2), dma(2), dma(2, HI - 1), dma(2, HI - 1), dma(2), dma(2),
        dma(R - 1), dma(R - 1), dma(C - 1), dma(C - 1),
    ]
    spec = pl.BlockSpec(memory_space=vmem)
    results = (((2, F, H), f32), ((2, A, F), f32), ((2, H), f32), ((2, F, H), f32),
               ((2, A, F), f32), ((2, H), f32), ((2, TB), f32), ((TB, A), f32))
    kept = pl.pallas_call(
        functools.partial(kernel, dims),
        out_shape=tuple(vmem(shape, kind) for shape, kind in results),
        in_specs=[pl.BlockSpec(memory_space=pltpu.HBM)] * 14,
        out_specs=(spec,) * len(results),
        scratch_shapes=scratch,
        compiler_params=pltpu.CompilerParams(
            collective_id=0, has_side_effects=True, vmem_limit_bytes=57 * 2 ** 20),
    )(*[pltpu.with_memory_space_constraint(one, pltpu.HBM) for one in (
        observed, next_observed, actions, next_mean, policy_noise, rewards[None, :],
        discounts[None, :], actor_flags[None, :], critic_in, critic_act, critic_head, target_in,
        target_act, target_head)])
    return pl.pallas_call(
        put_out,
        out_shape=tuple(jax.ShapeDtypeStruct(shape, kind) for shape, kind in results),
        in_specs=[spec] * len(results),
        out_specs=(pl.BlockSpec(memory_space=pl.ANY),) * len(results),
        scratch_shapes=[dma(len(results))],
        compiler_params=pltpu.CompilerParams(vmem_limit_bytes=12 * 2 ** 20),
    )(*[pltpu.with_memory_space_constraint(one, vmem) for one in kept])


def solution(mesh):
    def run(*args):
        R, C, D = mesh.shape["row"], mesh.shape["col"], mesh.shape["dp"]
        tokens, features = args[0].shape
        dims = (R, C, D, tokens // (R * D), features // C, args[8].shape[2] // R,
                args[2].shape[1])
        return sharded(dims)(*args)

    def sharded(dims):
        return jax.shard_map(
            functools.partial(on_device, dims),
            mesh=mesh,
            in_specs=(
                P(("row", "dp"), "col"),
                P(("row", "dp"), "col"),
                P(("row", "dp"), None),
                P(("row", "dp"), None),
                P(("row", "dp"), None),
                P(("row", "dp")),
                P(("row", "dp")),
                P(("row", "dp")),
                P(None, "col", "row"),
                P(None, None, "col"),
                P(None, "row"),
                P(None, "col", "row"),
                P(None, None, "col"),
                P(None, "row"),
            ),
            out_specs=(
                P(None, "col", "row"),
                P(None, None, "col"),
                P(None, "row"),
                P(None, "col", "row"),
                P(None, None, "col"),
                P(None, "row"),
                P(None, ("row", "dp")),
                P(("row", "dp"), None),
            ),
            check_vma=False,
        )

    return run
```

```python
import functools

import jax
import jax.numpy as jnp
from jax import lax
from jax.experimental import pallas as pl
from jax.experimental.pallas import tpu as pltpu
from jax.sharding import PartitionSpec as P

noise_clip = 0.5
matrix_rate = 0.004
head_rate = 0.0001
blend_rate = 0.005

f32 = jnp.float32
bf16 = jnp.bfloat16
pace = 5
lead = 2
cuts = 2
pieces = 2


def kernel(dims, observed_at, next_observed_at, actions_at, next_mean_at, noise_at, rewards_at,
           discounts_at, flags_at, cin_at, cact_at, chead_at, tin_at, tact_at, thead_at,
           new_in, new_act, new_head, new_tin, new_tact, new_thead, errs_out, push_out,
           next_mean, noise, rewards, discounts, flags, cin, cact, chead, tin, tact, thead,
           on_own, tg_own, flag_column, w16, a16, on_all, tg_all, emb, slopes, turned, lift,
           sums_out, sums_in, mine, hidden, vals_t, vals_o, rd_own, rd_all, vt_all, vo_all, gl,
           err_own, err_top, gh, epad, columns,
           ga_own, ga_out, ga_in, gb_all, gc_all, pu_out, pu_in, pz_all,
           load_s, on_s, on_r, tg_s, tg_r, ftg_s, ftg_r, ox_s, ox_r, oo_s, oo_r, rd_s, rd_r,
           sm_s, sm_r, xs_s, xs_r, vt_s, vt_r, vo_s, vo_r, gl_s, gl_r, er_s, er_r,
           gh_s, gh_r, ga_s, ga_r, gb_s, gb_r, gc_s, gc_r, pu_s, pu_r, pz_s, pz_r):
    R, C, D, TB, F, H, A = dims
    HI = R // 2
    TC = TB // pieces
    row, col, dp = lax.axis_index("row"), lax.axis_index("col"), lax.axis_index("dp")
    hi, lo = row // 2, row % 2
    nt = 2 * HI * pieces
    no = 2 * R * pieces
    n = nt + no
    partner = hi * 2 + (1 - lo)

    def copy(src, dst, ssem, rsem, **where):
        return pltpu.make_async_remote_copy(
            src_ref=src, dst_ref=dst, send_sem=ssem, recv_sem=rsem,
            device_id=where, device_id_type=pl.DeviceIdType.MESH)

    def bulk(region, ssem, rsem):
        return copy(region, region, ssem, rsem, row=partner)

    pairs = [(next_observed_at, tg_own.at[:, :F]), (next_mean_at, next_mean), (noise_at, noise),
             (tact_at, tact), (tin_at.at[0], tin.at[0]), (tin_at.at[1], tin.at[1]),
             (thead_at, thead), (observed_at, on_own.at[:, :F]), (actions_at, on_own.at[:, F:]),
             (rewards_at, rewards), (discounts_at, discounts), (flags_at, flags),
             (cact_at, cact), (cin_at.at[0], cin.at[0]), (cin_at.at[1], cin.at[1]),
             (chead_at, chead)]
    loads = [pltpu.make_async_copy(src, dst, load_s.at[x]) for x, (src, dst) in enumerate(pairs)]
    for load in loads:
        load.start()

    plane = [(c, d) for d in range(D) for c in range(C) if c or d]
    group = [(r, d) for d in range(D) for r in range(R) if r or d]
    others = [(r, 0, d) for r, d in group] + [(0, c, d) for c, d in plane if c]
    barrier = pltpu.get_barrier_semaphore()
    for r, c, d in others:
        pl.semaphore_signal(barrier, inc=1,
                            device_id={"row": (row + r) % R, "col": (col + c) % C,
                                       "dp": (dp + d) % D},
                            device_id_type=pl.DeviceIdType.MESH)

    vals_t[...] = jnp.zeros_like(vals_t)
    vals_o[...] = jnp.zeros_like(vals_o)
    for x in range(3):
        loads[x].wait()
    tg_own[:, F:] = jnp.clip(
        next_mean[...].astype(f32) + jnp.clip(noise[...], -noise_clip, noise_clip), -1.0, 1.0
    ).astype(bf16)
    pl.semaphore_wait(barrier, len(others))

    def tg_copy(o):
        to = partner if o == 0 else ((hi + o) % HI) * 2 + lo
        return copy(tg_own, tg_all.at[row], tg_s.at[o], tg_r.at[o], row=to)

    def ftg_copy(o, block):
        return copy(tg_all.at[block], tg_all.at[block], ftg_s.at[o], ftg_r.at[o], row=partner)

    def on_copy(o):
        return copy(on_own, on_all.at[dp, row], on_s.at[o - 1], on_r.at[o - 1],
                    row=(row + o) % R)

    def ox_copy(e):
        return copy(on_own, on_all.at[dp, row], ox_s.at[e - 1], ox_r.at[e - 1], dp=(dp + e) % D)

    def oo_copy(e, o):
        at = on_all.at[(dp + D - e) % D, row]
        return copy(at, at, oo_s.at[e - 1, o - 1], oo_r.at[e - 1, o - 1], row=(row + o) % R)

    def rd_copy(o):
        return copy(rd_own, rd_all.at[row], rd_s.at[0], rd_r.at[0], row=(row + o) % R)

    for o in range(HI):
        tg_copy(o).start()
    tg_all[row] = tg_own[...]
    for x in range(9, 11):
        loads[x].wait()
    rd_own[...] = jnp.zeros_like(rd_own)
    rd_own[0:1, :] = rewards[...].astype(f32)
    rd_own[1:2, :] = discounts[...].astype(f32)
    for o in range(1, R):
        rd_copy(o).start()
    rd_all[row] = rd_own[...]
    for x in range(3, 7):
        loads[x].wait()
    for k in range(2):
        a16[2 + k] = tact[k].astype(bf16)
    w16[2] = tin[0].astype(bf16)

    def rows_of(d, block):
        return pl.ds(pl.multiple_of((d * R + block) * TB, TB), TB)

    def embed_on(d, block):
        x = on_all[d, block]
        turned[:, rows_of(d, block)] = x[:, F:].T
        for k in range(2):
            mixed = jnp.dot(x[:, F:], a16[k], preferred_element_type=f32)
            emb[k, rows_of(d, block), :] = (x[:, :F].astype(f32) + mixed).astype(bf16)

    def embed_tg(block):
        x = tg_all[block]
        for k in range(2):
            mixed = jnp.dot(x[:, F:], a16[2 + k], preferred_element_type=f32)
            emb[k, rows_of(D, block), :] = (x[:, :F].astype(f32) + mixed).astype(bf16)

    def prepare_tg(a, i):
        for o in range(HI):
            block = ((hi + HI - o) % HI) * 2 + a

            @pl.when(i == 2 * pieces * o)
            def _():
                @pl.when(lo != a)
                def _():
                    if o > 0:
                        ftg_copy(o, block).wait_recv()
                    else:
                        tg_copy(0).wait_recv()
                embed_tg(block)

    def forward_tg(a, i, far):
        for o in range(1, HI):
            @pl.when((i == 2 * pieces * o - jnp.where(far == 0, 1, pieces + 1)) & (lo == a))
            def _():
                tg_copy(o).wait_recv()
                ftg_copy(o, ((hi + HI - o) % HI) * 2 + a).start()

    def prepare_on(q):
        for o in range(R):
            @pl.when(q == 2 * pieces * o)
            def _():
                if o > 0:
                    on_copy(o).wait_recv()
                embed_on(dp, (row + R - o) % R)

    def along(a):
        return jnp.where(a == 0, col + 1, col + C - 1) % C

    def sm_copy(a, i):
        return copy(sums_out.at[a, i], sums_in.at[a, i], sm_s.at[a], sm_r.at[a, i], col=along(a))

    def sm_sent(a):
        return copy(sums_out.at[a], sums_in.at[a], sm_s.at[a], sm_r.at[a, 0], col=along(a))

    def place_t(a, i):
        block = ((hi + HI - i // (2 * pieces)) % HI) * 2 + a
        return block, (i // pieces) % 2, i % pieces

    def place_o(q):
        return (row + R - q // (2 * pieces)) % R, (q // pieces) % 2, q % pieces

    def chunk(d, block, piece):
        return pl.ds(pl.multiple_of((d * R + block) * TB + piece * TC, TC), TC)

    def xs_copy(q, e):
        block, kk, piece = place_o(q)
        at = slopes.at[kk, chunk(dp, block, piece), :]
        return copy(at, at, xs_s.at[kk, e - 1], xs_r.at[kk, e - 1], dp=(dp + e) % D)

    def xs_whole(k, e):
        at = slopes.at[k, pl.ds(pl.multiple_of(dp * R * TB, R * TB), R * TB), :]
        return copy(at, at, xs_s.at[k, e - 1], xs_r.at[k, e - 1], dp=(dp + e) % D)

    def vt_copy(o):
        return copy(vt_all.at[row], vt_all.at[row], vt_s.at[0], vt_r.at[0],
                    row=(row + o) % R)

    def gl_copy(x, a):
        c, d = plane[x]
        at = gl.at[dp * 2 + a]
        return copy(at, at, gl_s.at[x], gl_r.at[0],
                    col=(col + c) % C, dp=(dp + d) % D)

    def vo_copy(x):
        r, d = group[x]
        at = vo_all.at[dp * R + row]
        return copy(at, at, vo_s.at[0], vo_r.at[0],
                    row=(row + r) % R, dp=(dp + d) % D)

    lane = lax.broadcasted_iota(jnp.int32, (TC, 128), 1)

    def note(store, block, kk, piece, gate, head):
        value = jnp.sum(gate * head, axis=1, keepdims=True)
        at = pl.ds(pl.multiple_of(piece * TC, TC), TC)
        store[at, :] += jnp.where(lane == kk * R + block, value, 0.0)

    def finish_t(a, i, pre):
        block, kk, piece = place_t(a, i)
        note(vals_t, block, kk, piece, pre * jax.nn.sigmoid(pre), thead[pl.ds(kk, 1), :])

    def finish_o(q, pre):
        block, kk, piece = place_o(q)
        sigma = jax.nn.sigmoid(pre)
        gate = pre * sigma
        head = chead[pl.ds(kk, 1), :]
        slopes[kk, chunk(dp, block, piece), :] = (
            head * (sigma * (1.0 + pre * (1.0 - sigma)))).astype(bf16)
        hidden[kk, chunk(0, block, piece), :] = gate.astype(bf16)
        note(vals_o, block, kk, piece, gate, head)

        @pl.when(q == no - 1)
        def _():
            vo_all[dp * R + row] = vals_o[...].T[:2 * R]
            for x in range(len(group)):
                vo_copy(x).start()
        for e in range(1, D):
            xs_copy(q, e).start()

    def settle(a, i):
        @pl.when(i == nt)
        def _():
            vt_all[row] = vals_t[...].T[:2 * R]
            for o in range(1, R):
                vt_copy(o).start()

        @pl.when(i == nt + 2 * pieces - 1)
        def _():
            bulk(vt_all.at[:R - 1], vt_s.at[0], vt_r.at[0]).wait_recv()
            total = vt_all[0]
            for r in range(1, R):
                total = total + vt_all[r]
            reward = jnp.concatenate([rd_all[b, 0:1] for b in range(R)], axis=0)
            discount = jnp.concatenate([rd_all[b, 1:2] for b in range(R)], axis=0)
            goal = reward + discount * jnp.minimum(total[:R], total[R:])
            mine = lax.broadcasted_iota(jnp.int32, (R, TB), 0) % 2 == a
            goal = jnp.where(mine, goal, 0.0)
            gl[dp * 2 + a] = jnp.concatenate([goal, goal], axis=0)
            for x in range(len(plane)):
                gl_copy(x, a).start()

    def later(a, far):
        return 2 * far + a > C - 1

    steps = n + lead + pace * (C - 1) // 2

    def aside(s):
        @pl.when(s == 0)
        def _():
            w16[3] = tin[1].astype(bf16)
            for x in (7, 8):
                loads[x].wait()
            for e in range(1, D):
                ox_copy(e).start()
            for o in range(1, R):
                on_copy(o).start()
            on_all[dp, row] = on_own[...]

        @pl.when(s == 1)
        def _():
            for x in range(11, 16):
                loads[x].wait()
            for k in range(2):
                a16[k] = cact[k].astype(bf16)
                w16[k] = cin[k].astype(bf16)

        @pl.when(s == nt)
        def _():
            bulk(rd_all.at[:R - 1], rd_s.at[0], rd_r.at[0]).wait_recv()

        @pl.when(s == nt + 2)
        def _():
            for e in range(1, D):
                ox_copy(e).wait_recv()
                for o in range(1, R):
                    oo_copy(e, o).start()

        @pl.when(s == nt + 1)
        def _():
            lift[...] = jnp.dot(a16[0], w16[0], preferred_element_type=f32).astype(bf16)

        for e in range(1, D):
            for o in range(R):
                @pl.when(s == nt + no // 2 + (e - 1) * R + o)
                def _():
                    if o > 0:
                        oo_copy(e, o).wait_recv()
                    embed_on((dp + D - e) % D, (row + R - o) % R)

    def step(s, carry):
        at = []
        for j in range(2):
            a = (col + j) % 2
            far = jnp.where(a == 0, col, C - 1 - col)
            i = s - pace * far // 2 - jnp.where(far > 0, lead, 0)
            at.append((a, far, i, (i >= 0) & (i < n)))

        for a, far, i, live in at:
            @pl.when(live)
            def _():
                early = i < nt
                q = i - nt
                tb, tk, tp = place_t(a, i)
                ob, ok, op = place_o(jnp.maximum(q, 0))
                kk = jnp.where(early, tk, ok)
                start = (jnp.where(early, D * R + tb, dp * R + ob) * TB
                         + jnp.where(early, tp, op) * TC)

                @pl.when(early)
                def _():
                    prepare_tg(a, i)

                @pl.when((q >= 0) & jnp.logical_not(later(a, far)))
                def _():
                    prepare_on(q)
                mine[a] = jnp.dot(emb[kk, pl.ds(pl.multiple_of(start, TC), TC), :],
                                  w16[jnp.where(early, 2, 0) + kk],
                                  preferred_element_type=f32)

        for a, far, i, live in at:
            @pl.when(live & (far == 0))
            def _():
                sums_out[a, i] = mine[a].astype(bf16)
                sm_copy(a, i).start()

        for a, far, i, live in at:
            @pl.when(live & (far > 0) & (far < C - 1))
            def _():
                sm_copy(a, i).wait_recv()
                total = mine[a] + sums_in[a, i].astype(f32)
                sums_out[a, i] = total.astype(bf16)
                sm_copy(a, i).start()
                mine[a] = total

            @pl.when(live & (far == C - 1))
            def _():
                sm_copy(a, i).wait_recv()
                mine[a] += sums_in[a, i].astype(f32)

        for a, far, i, live in at:
            @pl.when(live & (i < nt))
            def _():
                @pl.when(far == C - 1)
                def _():
                    finish_t(a, i, mine[a])
                forward_tg(a, i, far)

            @pl.when(live & (i >= nt) & later(a, far))
            def _():
                @pl.when(far < C - 1)
                def _():
                    mine[a] += sums_in[1 - a, i].astype(f32)
                finish_o(i - nt, mine[a])

            @pl.when(far == C - 1)
            def _():
                settle(a, i)
        aside(s)
        return carry

    lax.fori_loop(0, steps, step, 0)

    def pu_copy(o):
        return copy(pu_out.at[o - 1], pu_in.at[o - 1], pu_s.at[0], pu_r.at[0],
                    row=(row + o) % R)

    def pz_copy(c):
        return copy(pz_all.at[col], pz_all.at[col], pz_s.at[0], pz_r.at[0],
                    col=(col + c) % C)

    last = (((1,), (1,)), ((), ()))
    first = (((0,), (0,)), ((), ()))
    for o in list(range(1, R)) + [0]:
        got = lax.dot_general(slopes[0, rows_of(dp, (row + o) % R), :], lift[...], last,
                              preferred_element_type=f32)
        if o == 0:
            push_out[...] = got
        else:
            pu_out[o - 1] = got.astype(bf16)
            pu_copy(o).start()

    ends = (col == 0) | (col == C - 1)

    @pl.when(ends)
    def _():
        bulk(gl.at[:2 * D - 1], gl_s.at[0], gl_r.at[0]).wait_recv()

    @pl.when(jnp.logical_not(ends))
    def _():
        bulk(gl, gl_s.at[0], gl_r.at[0]).wait_recv()

    bulk(vo_all.at[:D * R - 1], vo_s.at[0], vo_r.at[0]).wait_recv()

    epad[...] = jnp.zeros_like(epad)
    for d in range(D):
        value = vo_all[d * R]
        for r in range(1, R):
            value = value + vo_all[d * R + r]
        err = value - (gl[2 * d] + gl[2 * d + 1])
        err_own[d] = err
        epad[:2 * R, :] = 2.0 * err
        columns[d] = epad[...].T

    F2 = F // 2

    def ga_copy(k):
        return copy(ga_out.at[k, 1 - lo], ga_in.at[k], ga_s.at[k], ga_r.at[k], row=partner)

    def gb_copy(k, o):
        return copy(gb_all.at[k, hi], gb_all.at[k, hi], gb_s.at[k, o - 1], gb_r.at[k, o - 1],
                    row=((hi + o) % HI) * 2 + lo)

    def gc_copy(k):
        return copy(gc_all.at[k, lo], gc_all.at[k, lo], gc_s.at[k], gc_r.at[k], row=partner)

    chief = 1 % C

    def er_copy(c):
        return copy(err_top, err_top, er_s.at[c - 1], er_r.at[0], col=(col + c) % C)

    def gh_copy(x):
        c, d = plane[x]
        return copy(gh.at[dp], gh.at[dp], gh_s.at[x], gh_r.at[0],
                    col=(col + c) % C, dp=(dp + d) % D)

    slot = lax.broadcasted_iota(jnp.int32, (2 * R, H), 0)

    @pl.when(col == chief)
    def _():
        err_top[...] = err_own[dp]
        for c in range(1, C):
            er_copy(c).start()
        twice = (2.0 * err_own[dp]).astype(bf16)
        total = jnp.zeros((2 * R, H), f32)
        for k in range(2):
            for b in range(R):
                got = jnp.dot(twice, hidden[k, b * TB:(b + 1) * TB, :],
                              preferred_element_type=f32)
                total = total + jnp.where(slot == k * R + b, got, 0.0)
        gh[dp] = total
        for x in range(len(plane)):
            gh_copy(x).start()

    for k in range(2):
        for e in range(1, D):
            xs_whole(k, e).wait()
        moved = jnp.zeros((A, H), f32)
        for d in range(D):
            for b in range(R):
                at = slice((d * R + b) * TB, (d * R + b + 1) * TB)
                slopes[k, at, :] = (columns[d, :, k * R + b:k * R + b + 1]
                                    * slopes[k, at, :].astype(f32)).astype(bf16)
            at = slice(d * R * TB, (d + 1) * R * TB)
            moved = moved + jnp.dot(turned[:, at], slopes[k, at, :],
                                    preferred_element_type=f32)
        term = lax.dot_general(moved.astype(bf16), w16[k], last, preferred_element_type=f32)

        for p in range(2):
            ga_own[k, p] = term[:, p * F2:(p + 1) * F2]
            ga_out[k, p] = term[:, p * F2:(p + 1) * F2].astype(bf16)
        ga_copy(k).start()

    for k in range(2):
        ga_copy(k).wait_recv()
        gb_all[k, hi] = (ga_own[k, lo] + ga_in[k].astype(f32)).astype(bf16)
        for o in range(1, HI):
            gb_copy(k, o).start()

    bulk(pu_in, pu_s.at[0], pu_r.at[0]).wait_recv()
    for o in range(1, R):
        push_out[...] += pu_in[o - 1].astype(f32)
    pz_all[col] = push_out[...].astype(bf16)
    for c in range(1, C):
        pz_copy(c).start()

    def blend(fresh, target):
        return blend_rate * fresh + (1.0 - blend_rate) * target

    def grad_in(k):
        def part(d):
            at = pl.ds(pl.multiple_of(d * R * TB, R * TB), R * TB)
            return lax.dot_general(emb[k, at, :], slopes[k, at, :], first,
                                   preferred_element_type=f32)

        def add(d, carry):
            new_in[k] += part(d)
            return carry
        new_in[k] = part(0)
        lax.fori_loop(1, D, add, 0)
        fresh = cin[k] - matrix_rate * new_in[k]
        new_in[k] = fresh
        new_tin[k] = blend(fresh, tin[k])

    grad_in(0)
    grad_in(1)

    for k in range(2):
        for o in range(1, HI):
            gb_copy(k, o).wait_recv()
        piece = gb_all[k, 0].astype(f32)
        for h in range(1, HI):
            piece = piece + gb_all[k, h].astype(f32)
        gc_all[k, lo] = piece.astype(bf16)
        gc_copy(k).start()

    bulk(pz_all.at[:C - 1], pz_s.at[0], pz_r.at[0]).wait_recv()
    push = pz_all[0].astype(f32)
    for c in range(1, C):
        push = push + pz_all[c].astype(f32)
    epad[0:1, :] = flags[...].astype(f32)
    flag_column[...] = epad[...].T[:, 0:1]
    push_out[...] = push * flag_column[...]

    @pl.when(col != chief)
    def _():
        er_copy(1).wait_recv()
    for k in range(2):
        errs_out[k:k + 1, :] = err_top[pl.ds(k * R + row, 1), :]

    @pl.when(col != chief)
    def _():
        bulk(gh, gh_s.at[0], gh_r.at[0]).wait_recv()

    @pl.when(col == chief)
    def _():
        bulk(gh.at[:D - 1], gh_s.at[0], gh_r.at[0]).wait_recv()
    whole = gh[0]
    for d in range(1, D):
        whole = whole + gh[d]
    for k in range(2):
        grad = jnp.sum(whole[k * R:(k + 1) * R], axis=0, keepdims=True)
        fresh = chead[k:k + 1, :] - head_rate * grad
        new_head[k:k + 1, :] = fresh
        new_thead[k:k + 1, :] = blend(fresh, thead[k:k + 1, :])

    for k in range(2):
        gc_copy(k).wait_recv()
        for p in range(2):
            part = slice(p * F2, (p + 1) * F2)
            fresh = cact[k, :, part] - matrix_rate * gc_all[k, p].astype(f32)
            new_act[k, :, part] = fresh
            new_tact[k, :, part] = blend(fresh, tact[k, :, part])

    for o in range(HI):
        tg_copy(o).wait_send()
        if o > 0:
            ftg_copy(o, row).wait_send()
    for o in range(1, R):
        on_copy(o).wait_send()
        for e in range(1, D):
            oo_copy(e, o).wait_send()
    for e in range(1, D):
        ox_copy(e).wait_send()
    for a in range(2):
        far = col if a == 0 else C - 1 - col

        @pl.when(far < C - 1)
        def _():
            sm_sent(a).wait_send()

        @pl.when(far == C - 1)
        def _():
            bulk(vt_all.at[:R - 1], vt_s.at[0], vt_r.at[0]).wait_send()
            for x in range(len(plane)):
                gl_copy(x, a).wait_send()

    bulk(vo_all.at[:D * R - 1], vo_s.at[0], vo_r.at[0]).wait_send()
    bulk(rd_all.at[:R - 1], rd_s.at[0], rd_r.at[0]).wait_send()
    bulk(pz_all.at[:C - 1], pz_s.at[0], pz_r.at[0]).wait_send()
    bulk(pu_out, pu_s.at[0], pu_r.at[0]).wait_send()

    @pl.when(col == chief)
    def _():
        for c in range(1, C):
            er_copy(c).wait_send()
        for x in range(len(plane)):
            gh_copy(x).wait_send()
    for k in range(2):
        ga_copy(k).wait_send()
        gc_copy(k).wait_send()
        for o in range(1, HI):
            gb_copy(k, o).wait_send()


def put_out(*refs):
    count = len(refs) // 2
    pairs = []
    for x in range(count):
        if len(refs[x].shape) == 3:
            rows = refs[x].shape[1] // cuts
            pairs += [(refs[x].at[k, c * rows:(c + 1) * rows],
                       refs[count + x].at[k, c * rows:(c + 1) * rows])
                      for k in range(2) for c in range(cuts)]
        else:
            pairs.append((refs[x], refs[count + x]))
    copies = [pltpu.make_async_copy(src, dst, refs[-1].at[x])
              for x, (src, dst) in enumerate(pairs)]
    for one in copies:
        one.start()
    for one in copies:
        one.wait()


def on_device(dims, observed, next_observed, actions, next_mean, policy_noise, rewards, discounts,
              actor_flags, critic_in, critic_act, critic_head, target_in, target_act, target_head):
    R, C, D, TB, F, H, A = dims
    HI, TC = R // 2, TB // pieces
    nt, no = 2 * HI * pieces, 2 * R * pieces
    planes = C * D - 1
    dma = lambda *shape: pltpu.SemaphoreType.DMA(shape)
    vmem = pltpu.VMEM
    scratch = [
        vmem((TB, A), bf16), vmem((TB, A), f32), vmem((1, TB), bf16), vmem((1, TB), bf16),
        vmem((1, TB), jnp.int32), vmem((2, F, H), f32), vmem((2, A, F), f32), vmem((2, H), f32),
        vmem((2, F, H), f32), vmem((2, A, F), f32), vmem((2, H), f32),
        vmem((TB, F + A), bf16), vmem((TB, F + A), bf16), vmem((TB, 1), f32),
        vmem((4, F, H), bf16), vmem((4, A, F), bf16),
        vmem((D, R, TB, F + A), bf16), vmem((R, TB, F + A), bf16),
        vmem((2, (D + 1) * R * TB, F), bf16),
        vmem((2, D * R * TB, H), bf16), vmem((A, D * R * TB), bf16), vmem((A, H), bf16),
        vmem((2, nt + no, TC, H), bf16), vmem((2, nt + no, TC, H), bf16), vmem((2, TC, H), f32),
        vmem((2, R * TB, H), bf16), vmem((TB, 128), f32), vmem((TB, 128), f32),
        vmem((8, TB), f32), vmem((R, 8, TB), f32), vmem((R, 2 * R, TB), f32),
        vmem((D * R, 2 * R, TB), f32), vmem((D * 2, 2 * R, TB), f32),
        vmem((D, 2 * R, TB), f32), vmem((2 * R, TB), f32), vmem((D, 2 * R, H), f32),
        vmem((128, TB), f32), vmem((D, TB, 128), f32),
        vmem((2, 2, A, F // 2), f32), vmem((2, 2, A, F // 2), bf16), vmem((2, A, F // 2), bf16),
        vmem((2, HI, A, F // 2), bf16), vmem((2, 2, A, F // 2), bf16),
        vmem((R - 1, TB, A), bf16), vmem((R - 1, TB, A), bf16), vmem((C, TB, A), bf16),
        dma(16),
        dma(R - 1), dma(R - 1), dma(HI), dma(HI), dma(HI), dma(HI),
        dma(D - 1), dma(D - 1), dma(D - 1, R - 1), dma(D - 1, R - 1), dma(1), dma(1),
        dma(2), dma(2, nt + no), dma(2, D - 1), dma(2, D - 1),
        dma(1), dma(1), dma(1), dma(1), dma(planes), dma(1),
        dma(C - 1), dma(1), dma(planes), dma(1),
        dma(2), dma(2), dma(2, HI - 1), dma(2, HI - 1), dma(2), dma(2),
        dma(1), dma(1), dma(1), dma(1),
    ]
    spec = pl.BlockSpec(memory_space=vmem)
    results = (((2, F, H), f32), ((2, A, F), f32), ((2, H), f32), ((2, F, H), f32),
               ((2, A, F), f32), ((2, H), f32), ((2, TB), f32), ((TB, A), f32))
    kept = pl.pallas_call(
        functools.partial(kernel, dims),
        out_shape=tuple(vmem(shape, kind) for shape, kind in results),
        in_specs=[pl.BlockSpec(memory_space=pltpu.HBM)] * 14,
        out_specs=(spec,) * len(results),
        scratch_shapes=scratch,
        compiler_params=pltpu.CompilerParams(
            collective_id=0, has_side_effects=True, vmem_limit_bytes=57 * 2 ** 20),
    )(*[pltpu.with_memory_space_constraint(one, pltpu.HBM) for one in (
        observed, next_observed, actions, next_mean, policy_noise, rewards[None, :],
        discounts[None, :], actor_flags[None, :], critic_in, critic_act, critic_head, target_in,
        target_act, target_head)])
    return pl.pallas_call(
        put_out,
        out_shape=tuple(jax.ShapeDtypeStruct(shape, kind) for shape, kind in results),
        in_specs=[spec] * len(results),
        out_specs=(pl.BlockSpec(memory_space=pl.ANY),) * len(results),
        scratch_shapes=[dma(8 * cuts + 4)],
        compiler_params=pltpu.CompilerParams(vmem_limit_bytes=12 * 2 ** 20),
    )(*[pltpu.with_memory_space_constraint(one, vmem) for one in kept])


def solution(mesh):
    def run(*args):
        R, C, D = mesh.shape["row"], mesh.shape["col"], mesh.shape["dp"]
        tokens, features = args[0].shape
        dims = (R, C, D, tokens // (R * D), features // C, args[8].shape[2] // R,
                args[2].shape[1])
        return sharded(dims)(*args)

    def sharded(dims):
        return jax.shard_map(
            functools.partial(on_device, dims),
            mesh=mesh,
            in_specs=(
                P(("row", "dp"), "col"),
                P(("row", "dp"), "col"),
                P(("row", "dp"), None),
                P(("row", "dp"), None),
                P(("row", "dp"), None),
                P(("row", "dp")),
                P(("row", "dp")),
                P(("row", "dp")),
                P(None, "col", "row"),
                P(None, None, "col"),
                P(None, "row"),
                P(None, "col", "row"),
                P(None, None, "col"),
                P(None, "row"),
            ),
            out_specs=(
                P(None, "col", "row"),
                P(None, None, "col"),
                P(None, "row"),
                P(None, "col", "row"),
                P(None, None, "col"),
                P(None, "row"),
                P(None, ("row", "dp")),
                P(("row", "dp"), None),
            ),
            check_vma=False,
        )

    return run
```

```python
import functools

import jax
import jax.numpy as jnp
from jax import lax
from jax.experimental import pallas as pl
from jax.experimental.pallas import tpu as pltpu
from jax.sharding import PartitionSpec as P

noise_clip = 0.5
matrix_rate = 0.004
head_rate = 0.0001
blend_rate = 0.005

f32 = jnp.float32
bf16 = jnp.bfloat16
pace = 5
lead = 2
cuts = 2
pieces = 2


def kernel(dims, observed_at, next_observed_at, actions_at, next_mean_at, noise_at, rewards_at,
           discounts_at, flags_at, cin_at, cact_at, chead_at, tin_at, tact_at, thead_at,
           new_in, new_act, new_head, new_tin, new_tact, new_thead, errs_out, push_out,
           next_mean, noise, rewards, discounts, flags, cin, cact, chead, tin, tact, thead,
           on_own, tg_own, flag_column, w16, a16, on_all, tg_all, emb, slopes, turned, lift,
           sums_out, sums_in, mine, hidden, vals_t, vals_o, rd_own, rd_all, vt_all, vo_all, gl,
           err_own, err_top, gh, epad, columns,
           ga_own, ga_out, ga_in, gb_all, gc_all, pu_out, pu_in, pz_all,
           load_s, on_s, on_r, tg_s, tg_r, ftg_s, ftg_r, ox_s, ox_r, oo_s, oo_r, rd_s, rd_r,
           sm_s, sm_r, xs_s, xs_r, vt_s, vt_r, vo_s, vo_r, gl_s, gl_r, er_s, er_r,
           gh_s, gh_r, ga_s, ga_r, gb_s, gb_r, gc_s, gc_r, pu_s, pu_r, pz_s, pz_r):
    R, C, D, TB, F, H, A = dims
    HI = R // 2
    TC = TB // pieces
    row, col, dp = lax.axis_index("row"), lax.axis_index("col"), lax.axis_index("dp")
    hi, lo = row // 2, row % 2
    nt = 2 * HI * pieces
    no = 2 * R * pieces
    n = nt + no
    partner = hi * 2 + (1 - lo)

    def copy(src, dst, ssem, rsem, **where):
        return pltpu.make_async_remote_copy(
            src_ref=src, dst_ref=dst, send_sem=ssem, recv_sem=rsem,
            device_id=where, device_id_type=pl.DeviceIdType.MESH)

    def bulk(region, ssem, rsem):
        return copy(region, region, ssem, rsem, row=partner)

    pairs = [(next_observed_at, tg_own.at[:, :F]), (next_mean_at, next_mean), (noise_at, noise),
             (tact_at, tact), (tin_at.at[0], tin.at[0]), (tin_at.at[1], tin.at[1]),
             (thead_at, thead), (observed_at, on_own.at[:, :F]), (actions_at, on_own.at[:, F:]),
             (rewards_at, rewards), (discounts_at, discounts), (flags_at, flags),
             (cact_at, cact), (cin_at.at[0], cin.at[0]), (cin_at.at[1], cin.at[1]),
             (chead_at, chead)]
    loads = [pltpu.make_async_copy(src, dst, load_s.at[x]) for x, (src, dst) in enumerate(pairs)]
    for load in loads:
        load.start()

    plane = [(c, d) for d in range(D) for c in range(C) if c or d]
    group = [(r, d) for d in range(D) for r in range(R) if r or d]
    others = [(r, 0, d) for r, d in group] + [(0, c, d) for c, d in plane if c]
    barrier = pltpu.get_barrier_semaphore()
    for r, c, d in others:
        pl.semaphore_signal(barrier, inc=1,
                            device_id={"row": (row + r) % R, "col": (col + c) % C,
                                       "dp": (dp + d) % D},
                            device_id_type=pl.DeviceIdType.MESH)

    vals_t[...] = jnp.zeros_like(vals_t)
    vals_o[...] = jnp.zeros_like(vals_o)
    for x in range(3):
        loads[x].wait()
    tg_own[:, F:] = jnp.clip(
        next_mean[...].astype(f32) + jnp.clip(noise[...], -noise_clip, noise_clip), -1.0, 1.0
    ).astype(bf16)
    pl.semaphore_wait(barrier, len(others))

    def tg_copy(o):
        to = partner if o == 0 else ((hi + o) % HI) * 2 + lo
        return copy(tg_own, tg_all.at[row], tg_s.at[o], tg_r.at[o], row=to)

    def ftg_copy(o, block):
        return copy(tg_all.at[block], tg_all.at[block], ftg_s.at[o], ftg_r.at[o], row=partner)

    def on_copy(o):
        return copy(on_own, on_all.at[dp, row], on_s.at[o - 1], on_r.at[o - 1],
                    row=(row + o) % R)

    def ox_copy(e):
        return copy(on_own, on_all.at[dp, row], ox_s.at[e - 1], ox_r.at[e - 1], dp=(dp + e) % D)

    def oo_copy(e, o):
        at = on_all.at[(dp + D - e) % D, row]
        return copy(at, at, oo_s.at[e - 1, o - 1], oo_r.at[e - 1, o - 1], row=(row + o) % R)

    def rd_copy(o):
        return copy(rd_own, rd_all.at[row], rd_s.at[0], rd_r.at[0], row=(row + o) % R)

    for o in range(HI):
        tg_copy(o).start()
    tg_all[row] = tg_own[...]
    for x in range(9, 11):
        loads[x].wait()
    rd_own[...] = jnp.zeros_like(rd_own)
    rd_own[0:1, :] = rewards[...].astype(f32)
    rd_own[1:2, :] = discounts[...].astype(f32)
    for o in range(1, R):
        rd_copy(o).start()
    rd_all[row] = rd_own[...]
    for x in range(3, 7):
        loads[x].wait()
    for k in range(2):
        a16[2 + k] = tact[k].astype(bf16)
    w16[2] = tin[0].astype(bf16)

    def rows_of(d, block):
        return pl.ds(pl.multiple_of((d * R + block) * TB, TB), TB)

    def embed_on(d, block):
        x = on_all[d, block]
        turned[:, rows_of(d, block)] = x[:, F:].T
        for k in range(2):
            mixed = jnp.dot(x[:, F:], a16[k], preferred_element_type=f32)
            emb[k, rows_of(d, block), :] = (x[:, :F].astype(f32) + mixed).astype(bf16)

    def embed_tg(block):
        x = tg_all[block]
        for k in range(2):
            mixed = jnp.dot(x[:, F:], a16[2 + k], preferred_element_type=f32)
            emb[k, rows_of(D, block), :] = (x[:, :F].astype(f32) + mixed).astype(bf16)

    def prepare_tg(a, i):
        for o in range(HI):
            block = ((hi + HI - o) % HI) * 2 + a

            @pl.when(i == 2 * pieces * o)
            def _():
                @pl.when(lo != a)
                def _():
                    if o > 0:
                        ftg_copy(o, block).wait_recv()
                    else:
                        tg_copy(0).wait_recv()
                embed_tg(block)

    def forward_tg(a, i, far):
        for o in range(1, HI):
            @pl.when((i == 2 * pieces * o - jnp.where(far == 0, 1, pieces + 1)) & (lo == a))
            def _():
                tg_copy(o).wait_recv()
                ftg_copy(o, ((hi + HI - o) % HI) * 2 + a).start()

    def prepare_on(q):
        for o in range(R):
            @pl.when(q == 2 * pieces * o)
            def _():
                if o > 0:
                    on_copy(o).wait_recv()
                embed_on(dp, (row + R - o) % R)

    def along(a):
        return jnp.where(a == 0, col + 1, col + C - 1) % C

    def sm_copy(a, i):
        return copy(sums_out.at[a, i], sums_in.at[a, i], sm_s.at[a], sm_r.at[a, i], col=along(a))

    def sm_sent(a):
        return copy(sums_out.at[a], sums_in.at[a], sm_s.at[a], sm_r.at[a, 0], col=along(a))

    def place_t(a, i):
        block = ((hi + HI - i // (2 * pieces)) % HI) * 2 + a
        return block, (i // pieces) % 2, i % pieces

    def place_o(q):
        return (row + R - q // (2 * pieces)) % R, (q // pieces) % 2, q % pieces

    def chunk(d, block, piece):
        return pl.ds(pl.multiple_of((d * R + block) * TB + piece * TC, TC), TC)

    def xs_copy(q, e):
        block, kk, piece = place_o(q)
        at = slopes.at[kk, chunk(dp, block, piece), :]
        return copy(at, at, xs_s.at[kk, e - 1], xs_r.at[kk, e - 1], dp=(dp + e) % D)

    def xs_whole(k, e):
        at = slopes.at[k, pl.ds(pl.multiple_of(dp * R * TB, R * TB), R * TB), :]
        return copy(at, at, xs_s.at[k, e - 1], xs_r.at[k, e - 1], dp=(dp + e) % D)

    def vt_copy(o):
        return copy(vt_all.at[row], vt_all.at[row], vt_s.at[0], vt_r.at[0],
                    row=(row + o) % R)

    def gl_copy(x, a):
        c, d = plane[x]
        at = gl.at[dp * 2 + a]
        return copy(at, at, gl_s.at[x], gl_r.at[0],
                    col=(col + c) % C, dp=(dp + d) % D)

    def vo_copy(x):
        r, d = group[x]
        at = vo_all.at[dp * R + row]
        return copy(at, at, vo_s.at[0], vo_r.at[0],
                    row=(row + r) % R, dp=(dp + d) % D)

    lane = lax.broadcasted_iota(jnp.int32, (TC, 128), 1)

    def note(store, block, kk, piece, gate, head):
        value = jnp.sum(gate * head, axis=1, keepdims=True)
        at = pl.ds(pl.multiple_of(piece * TC, TC), TC)
        store[at, :] += jnp.where(lane == kk * R + block, value, 0.0)

    def finish_t(a, i, pre):
        block, kk, piece = place_t(a, i)
        note(vals_t, block, kk, piece, pre * jax.nn.sigmoid(pre), thead[pl.ds(kk, 1), :])

    def finish_o(q, pre):
        block, kk, piece = place_o(q)
        sigma = jax.nn.sigmoid(pre)
        gate = pre * sigma
        head = chead[pl.ds(kk, 1), :]
        slopes[kk, chunk(dp, block, piece), :] = (
            head * (sigma * (1.0 + pre * (1.0 - sigma)))).astype(bf16)
        hidden[kk, chunk(0, block, piece), :] = gate.astype(bf16)
        note(vals_o, block, kk, piece, gate, head)

        @pl.when(q == no - 1)
        def _():
            vo_all[dp * R + row] = vals_o[...].T[:2 * R]
            for x in range(len(group)):
                vo_copy(x).start()
        for e in range(1, D):
            xs_copy(q, e).start()

    def settle(a, i):
        @pl.when(i == nt)
        def _():
            vt_all[row] = vals_t[...].T[:2 * R]
            for o in range(1, R):
                vt_copy(o).start()

        @pl.when(i == nt + 2 * pieces - 1)
        def _():
            bulk(vt_all.at[:R - 1], vt_s.at[0], vt_r.at[0]).wait_recv()
            total = vt_all[0]
            for r in range(1, R):
                total = total + vt_all[r]
            reward = jnp.concatenate([rd_all[b, 0:1] for b in range(R)], axis=0)
            discount = jnp.concatenate([rd_all[b, 1:2] for b in range(R)], axis=0)
            goal = reward + discount * jnp.minimum(total[:R], total[R:])
            mine = lax.broadcasted_iota(jnp.int32, (R, TB), 0) % 2 == a
            goal = jnp.where(mine, goal, 0.0)
            gl[dp * 2 + a] = jnp.concatenate([goal, goal], axis=0)
            for x in range(len(plane)):
                gl_copy(x, a).start()

    def later(a, far):
        return 2 * far + a > C - 1

    steps = n + lead + pace * (C - 1) // 2

    def aside(s):
        @pl.when(s == 0)
        def _():
            w16[3] = tin[1].astype(bf16)
            for x in (7, 8):
                loads[x].wait()
            for e in range(1, D):
                ox_copy(e).start()
            for o in range(1, R):
                on_copy(o).start()
            on_all[dp, row] = on_own[...]

        @pl.when(s == 1)
        def _():
            for x in range(11, 16):
                loads[x].wait()
            for k in range(2):
                a16[k] = cact[k].astype(bf16)
                w16[k] = cin[k].astype(bf16)

        @pl.when(s == nt)
        def _():
            bulk(rd_all.at[:R - 1], rd_s.at[0], rd_r.at[0]).wait_recv()

        @pl.when(s == nt + 2)
        def _():
            for e in range(1, D):
                ox_copy(e).wait_recv()
                for o in range(1, R):
                    oo_copy(e, o).start()

        @pl.when(s == nt + 1)
        def _():
            lift[...] = jnp.dot(a16[0], w16[0], preferred_element_type=f32).astype(bf16)

        for e in range(1, D):
            for o in range(R):
                @pl.when(s == nt + no // 2 + (e - 1) * R + o)
                def _():
                    if o > 0:
                        oo_copy(e, o).wait_recv()
                    embed_on((dp + D - e) % D, (row + R - o) % R)

    def step(s, carry):
        at = []
        for j in range(2):
            a = (col + j) % 2
            far = jnp.where(a == 0, col, C - 1 - col)
            i = s - pace * far // 2 - jnp.where(far > 0, lead, 0)
            at.append((a, far, i, (i >= 0) & (i < n)))

        for a, far, i, live in at:
            @pl.when(live)
            def _():
                early = i < nt
                q = i - nt
                tb, tk, tp = place_t(a, i)
                ob, ok, op = place_o(jnp.maximum(q, 0))
                kk = jnp.where(early, tk, ok)
                start = (jnp.where(early, D * R + tb, dp * R + ob) * TB
                         + jnp.where(early, tp, op) * TC)

                @pl.when(s == 0)
                def _():
                    prepare_tg(a, i)
                mine[a] = jnp.dot(emb[kk, pl.ds(pl.multiple_of(start, TC), TC), :],
                                  w16[jnp.where(early, 2, 0) + kk],
                                  preferred_element_type=f32)

        for a, far, i, live in at:
            @pl.when(live & (far == 0))
            def _():
                sums_out[a, i] = mine[a].astype(bf16)
                sm_copy(a, i).start()

        for a, far, i, live in at:
            @pl.when(live & (far > 0) & (far < C - 1))
            def _():
                sm_copy(a, i).wait_recv()
                total = mine[a] + sums_in[a, i].astype(f32)
                sums_out[a, i] = total.astype(bf16)
                sm_copy(a, i).start()
                mine[a] = total

            @pl.when(live & (far == C - 1))
            def _():
                sm_copy(a, i).wait_recv()
                mine[a] += sums_in[a, i].astype(f32)

        for a, far, i, live in at:
            @pl.when(live & (i < nt))
            def _():
                @pl.when(far == C - 1)
                def _():
                    finish_t(a, i, mine[a])
                forward_tg(a, i, far)

            @pl.when((s > 0) & (i == -1) | live & (i < nt - 1))
            def _():
                prepare_tg(a, i + 1)

            @pl.when((i >= nt - 1) & (i < n - 1) & jnp.logical_not(later(a, far)))
            def _():
                prepare_on(i + 1 - nt)

            @pl.when(live & (i >= nt) & later(a, far))
            def _():
                @pl.when(far < C - 1)
                def _():
                    mine[a] += sums_in[1 - a, i].astype(f32)
                finish_o(i - nt, mine[a])

            @pl.when(far == C - 1)
            def _():
                settle(a, i)
        aside(s)
        return carry

    lax.fori_loop(0, steps, step, 0)

    def pu_copy(o):
        return copy(pu_out.at[o - 1], pu_in.at[o - 1], pu_s.at[0], pu_r.at[0],
                    row=(row + o) % R)

    def pz_copy(c):
        return copy(pz_all.at[col], pz_all.at[col], pz_s.at[0], pz_r.at[0],
                    col=(col + c) % C)

    last = (((1,), (1,)), ((), ()))
    first = (((0,), (0,)), ((), ()))
    for o in list(range(1, R)) + [0]:
        got = lax.dot_general(slopes[0, rows_of(dp, (row + o) % R), :], lift[...], last,
                              preferred_element_type=f32)
        if o == 0:
            push_out[...] = got
        else:
            pu_out[o - 1] = got.astype(bf16)
            pu_copy(o).start()

    ends = (col == 0) | (col == C - 1)

    @pl.when(ends)
    def _():
        bulk(gl.at[:2 * D - 1], gl_s.at[0], gl_r.at[0]).wait_recv()

    @pl.when(jnp.logical_not(ends))
    def _():
        bulk(gl, gl_s.at[0], gl_r.at[0]).wait_recv()

    bulk(vo_all.at[:D * R - 1], vo_s.at[0], vo_r.at[0]).wait_recv()

    epad[...] = jnp.zeros_like(epad)
    for d in range(D):
        value = vo_all[d * R]
        for r in range(1, R):
            value = value + vo_all[d * R + r]
        err = value - (gl[2 * d] + gl[2 * d + 1])
        err_own[d] = err
        epad[:2 * R, :] = 2.0 * err
        columns[d] = epad[...].T

    F2 = F // 2

    def ga_copy(k):
        return copy(ga_out.at[k, 1 - lo], ga_in.at[k], ga_s.at[k], ga_r.at[k], row=partner)

    def gb_copy(k, o):
        return copy(gb_all.at[k, hi], gb_all.at[k, hi], gb_s.at[k, o - 1], gb_r.at[k, o - 1],
                    row=((hi + o) % HI) * 2 + lo)

    def gc_copy(k):
        return copy(gc_all.at[k, lo], gc_all.at[k, lo], gc_s.at[k], gc_r.at[k], row=partner)

    chief = 1 % C

    def er_copy(c):
        return copy(err_top, err_top, er_s.at[c - 1], er_r.at[0], col=(col + c) % C)

    def gh_copy(x):
        c, d = plane[x]
        return copy(gh.at[dp], gh.at[dp], gh_s.at[x], gh_r.at[0],
                    col=(col + c) % C, dp=(dp + d) % D)

    slot = lax.broadcasted_iota(jnp.int32, (2 * R, H), 0)

    @pl.when(col == chief)
    def _():
        err_top[...] = err_own[dp]
        for c in range(1, C):
            er_copy(c).start()
        twice = (2.0 * err_own[dp]).astype(bf16)
        total = jnp.zeros((2 * R, H), f32)
        for k in range(2):
            for b in range(R):
                got = jnp.dot(twice, hidden[k, b * TB:(b + 1) * TB, :],
                              preferred_element_type=f32)
                total = total + jnp.where(slot == k * R + b, got, 0.0)
        gh[dp] = total
        for x in range(len(plane)):
            gh_copy(x).start()

    for k in range(2):
        for e in range(1, D):
            xs_whole(k, e).wait()
        moved = jnp.zeros((A, H), f32)
        for d in range(D):
            for b in range(R):
                at = slice((d * R + b) * TB, (d * R + b + 1) * TB)
                slopes[k, at, :] = (columns[d, :, k * R + b:k * R + b + 1]
                                    * slopes[k, at, :].astype(f32)).astype(bf16)
            at = slice(d * R * TB, (d + 1) * R * TB)
            moved = moved + jnp.dot(turned[:, at], slopes[k, at, :],
                                    preferred_element_type=f32)
        term = lax.dot_general(moved.astype(bf16), w16[k], last, preferred_element_type=f32)

        for p in range(2):
            ga_own[k, p] = term[:, p * F2:(p + 1) * F2]
            ga_out[k, p] = term[:, p * F2:(p + 1) * F2].astype(bf16)
        ga_copy(k).start()

    for k in range(2):
        ga_copy(k).wait_recv()
        gb_all[k, hi] = (ga_own[k, lo] + ga_in[k].astype(f32)).astype(bf16)
        for o in range(1, HI):
            gb_copy(k, o).start()

    bulk(pu_in, pu_s.at[0], pu_r.at[0]).wait_recv()
    for o in range(1, R):
        push_out[...] += pu_in[o - 1].astype(f32)
    pz_all[col] = push_out[...].astype(bf16)
    for c in range(1, C):
        pz_copy(c).start()

    def blend(fresh, target):
        return blend_rate * fresh + (1.0 - blend_rate) * target

    def grad_in(k):
        def part(d):
            at = pl.ds(pl.multiple_of(d * R * TB, R * TB), R * TB)
            return lax.dot_general(emb[k, at, :], slopes[k, at, :], first,
                                   preferred_element_type=f32)

        def add(d, carry):
            new_in[k] += part(d)
            return carry
        new_in[k] = part(0)
        lax.fori_loop(1, D, add, 0)
        fresh = cin[k] - matrix_rate * new_in[k]
        new_in[k] = fresh
        new_tin[k] = blend(fresh, tin[k])

    grad_in(0)
    grad_in(1)

    for k in range(2):
        for o in range(1, HI):
            gb_copy(k, o).wait_recv()
        piece = gb_all[k, 0].astype(f32)
        for h in range(1, HI):
            piece = piece + gb_all[k, h].astype(f32)
        gc_all[k, lo] = piece.astype(bf16)
        gc_copy(k).start()

    bulk(pz_all.at[:C - 1], pz_s.at[0], pz_r.at[0]).wait_recv()
    push = pz_all[0].astype(f32)
    for c in range(1, C):
        push = push + pz_all[c].astype(f32)
    epad[0:1, :] = flags[...].astype(f32)
    flag_column[...] = epad[...].T[:, 0:1]
    push_out[...] = push * flag_column[...]

    @pl.when(col != chief)
    def _():
        er_copy(1).wait_recv()
    for k in range(2):
        errs_out[k:k + 1, :] = err_top[pl.ds(k * R + row, 1), :]

    @pl.when(col != chief)
    def _():
        bulk(gh, gh_s.at[0], gh_r.at[0]).wait_recv()

    @pl.when(col == chief)
    def _():
        bulk(gh.at[:D - 1], gh_s.at[0], gh_r.at[0]).wait_recv()
    whole = gh[0]
    for d in range(1, D):
        whole = whole + gh[d]
    for k in range(2):
        grad = jnp.sum(whole[k * R:(k + 1) * R], axis=0, keepdims=True)
        fresh = chead[k:k + 1, :] - head_rate * grad
        new_head[k:k + 1, :] = fresh
        new_thead[k:k + 1, :] = blend(fresh, thead[k:k + 1, :])

    for k in range(2):
        gc_copy(k).wait_recv()
        for p in range(2):
            part = slice(p * F2, (p + 1) * F2)
            fresh = cact[k, :, part] - matrix_rate * gc_all[k, p].astype(f32)
            new_act[k, :, part] = fresh
            new_tact[k, :, part] = blend(fresh, tact[k, :, part])

    for o in range(HI):
        tg_copy(o).wait_send()
        if o > 0:
            ftg_copy(o, row).wait_send()
    for o in range(1, R):
        on_copy(o).wait_send()
        for e in range(1, D):
            oo_copy(e, o).wait_send()
    for e in range(1, D):
        ox_copy(e).wait_send()
    for a in range(2):
        far = col if a == 0 else C - 1 - col

        @pl.when(far < C - 1)
        def _():
            sm_sent(a).wait_send()

        @pl.when(far == C - 1)
        def _():
            bulk(vt_all.at[:R - 1], vt_s.at[0], vt_r.at[0]).wait_send()
            for x in range(len(plane)):
                gl_copy(x, a).wait_send()

    bulk(vo_all.at[:D * R - 1], vo_s.at[0], vo_r.at[0]).wait_send()
    bulk(rd_all.at[:R - 1], rd_s.at[0], rd_r.at[0]).wait_send()
    bulk(pz_all.at[:C - 1], pz_s.at[0], pz_r.at[0]).wait_send()
    bulk(pu_out, pu_s.at[0], pu_r.at[0]).wait_send()

    @pl.when(col == chief)
    def _():
        for c in range(1, C):
            er_copy(c).wait_send()
        for x in range(len(plane)):
            gh_copy(x).wait_send()
    for k in range(2):
        ga_copy(k).wait_send()
        gc_copy(k).wait_send()
        for o in range(1, HI):
            gb_copy(k, o).wait_send()


def put_out(*refs):
    count = len(refs) // 2
    pairs = []
    for x in range(count):
        if len(refs[x].shape) == 3:
            rows = refs[x].shape[1] // cuts
            pairs += [(refs[x].at[k, c * rows:(c + 1) * rows],
                       refs[count + x].at[k, c * rows:(c + 1) * rows])
                      for k in range(2) for c in range(cuts)]
        else:
            pairs.append((refs[x], refs[count + x]))
    copies = [pltpu.make_async_copy(src, dst, refs[-1].at[x])
              for x, (src, dst) in enumerate(pairs)]
    for one in copies:
        one.start()
    for one in copies:
        one.wait()


def on_device(dims, observed, next_observed, actions, next_mean, policy_noise, rewards, discounts,
              actor_flags, critic_in, critic_act, critic_head, target_in, target_act, target_head):
    R, C, D, TB, F, H, A = dims
    HI, TC = R // 2, TB // pieces
    nt, no = 2 * HI * pieces, 2 * R * pieces
    planes = C * D - 1
    dma = lambda *shape: pltpu.SemaphoreType.DMA(shape)
    vmem = pltpu.VMEM
    scratch = [
        vmem((TB, A), bf16), vmem((TB, A), f32), vmem((1, TB), bf16), vmem((1, TB), bf16),
        vmem((1, TB), jnp.int32), vmem((2, F, H), f32), vmem((2, A, F), f32), vmem((2, H), f32),
        vmem((2, F, H), f32), vmem((2, A, F), f32), vmem((2, H), f32),
        vmem((TB, F + A), bf16), vmem((TB, F + A), bf16), vmem((TB, 1), f32),
        vmem((4, F, H), bf16), vmem((4, A, F), bf16),
        vmem((D, R, TB, F + A), bf16), vmem((R, TB, F + A), bf16),
        vmem((2, (D + 1) * R * TB, F), bf16),
        vmem((2, D * R * TB, H), bf16), vmem((A, D * R * TB), bf16), vmem((A, H), bf16),
        vmem((2, nt + no, TC, H), bf16), vmem((2, nt + no, TC, H), bf16), vmem((2, TC, H), f32),
        vmem((2, R * TB, H), bf16), vmem((TB, 128), f32), vmem((TB, 128), f32),
        vmem((8, TB), f32), vmem((R, 8, TB), f32), vmem((R, 2 * R, TB), f32),
        vmem((D * R, 2 * R, TB), f32), vmem((D * 2, 2 * R, TB), f32),
        vmem((D, 2 * R, TB), f32), vmem((2 * R, TB), f32), vmem((D, 2 * R, H), f32),
        vmem((128, TB), f32), vmem((D, TB, 128), f32),
        vmem((2, 2, A, F // 2), f32), vmem((2, 2, A, F // 2), bf16), vmem((2, A, F // 2), bf16),
        vmem((2, HI, A, F // 2), bf16), vmem((2, 2, A, F // 2), bf16),
        vmem((R - 1, TB, A), bf16), vmem((R - 1, TB, A), bf16), vmem((C, TB, A), bf16),
        dma(16),
        dma(R - 1), dma(R - 1), dma(HI), dma(HI), dma(HI), dma(HI),
        dma(D - 1), dma(D - 1), dma(D - 1, R - 1), dma(D - 1, R - 1), dma(1), dma(1),
        dma(2), dma(2, nt + no), dma(2, D - 1), dma(2, D - 1),
        dma(1), dma(1), dma(1), dma(1), dma(planes), dma(1),
        dma(C - 1), dma(1), dma(planes), dma(1),
        dma(2), dma(2), dma(2, HI - 1), dma(2, HI - 1), dma(2), dma(2),
        dma(1), dma(1), dma(1), dma(1),
    ]
    spec = pl.BlockSpec(memory_space=vmem)
    results = (((2, F, H), f32), ((2, A, F), f32), ((2, H), f32), ((2, F, H), f32),
               ((2, A, F), f32), ((2, H), f32), ((2, TB), f32), ((TB, A), f32))
    kept = pl.pallas_call(
        functools.partial(kernel, dims),
        out_shape=tuple(vmem(shape, kind) for shape, kind in results),
        in_specs=[pl.BlockSpec(memory_space=pltpu.HBM)] * 14,
        out_specs=(spec,) * len(results),
        scratch_shapes=scratch,
        compiler_params=pltpu.CompilerParams(
            collective_id=0, has_side_effects=True, vmem_limit_bytes=57 * 2 ** 20),
    )(*[pltpu.with_memory_space_constraint(one, pltpu.HBM) for one in (
        observed, next_observed, actions, next_mean, policy_noise, rewards[None, :],
        discounts[None, :], actor_flags[None, :], critic_in, critic_act, critic_head, target_in,
        target_act, target_head)])
    return pl.pallas_call(
        put_out,
        out_shape=tuple(jax.ShapeDtypeStruct(shape, kind) for shape, kind in results),
        in_specs=[spec] * len(results),
        out_specs=(pl.BlockSpec(memory_space=pl.ANY),) * len(results),
        scratch_shapes=[dma(8 * cuts + 4)],
        compiler_params=pltpu.CompilerParams(vmem_limit_bytes=12 * 2 ** 20),
    )(*[pltpu.with_memory_space_constraint(one, vmem) for one in kept])


def solution(mesh):
    def run(*args):
        R, C, D = mesh.shape["row"], mesh.shape["col"], mesh.shape["dp"]
        tokens, features = args[0].shape
        dims = (R, C, D, tokens // (R * D), features // C, args[8].shape[2] // R,
                args[2].shape[1])
        return sharded(dims)(*args)

    def sharded(dims):
        return jax.shard_map(
            functools.partial(on_device, dims),
            mesh=mesh,
            in_specs=(
                P(("row", "dp"), "col"),
                P(("row", "dp"), "col"),
                P(("row", "dp"), None),
                P(("row", "dp"), None),
                P(("row", "dp"), None),
                P(("row", "dp")),
                P(("row", "dp")),
                P(("row", "dp")),
                P(None, "col", "row"),
                P(None, None, "col"),
                P(None, "row"),
                P(None, "col", "row"),
                P(None, None, "col"),
                P(None, "row"),
            ),
            out_specs=(
                P(None, "col", "row"),
                P(None, None, "col"),
                P(None, "row"),
                P(None, "col", "row"),
                P(None, None, "col"),
                P(None, "row"),
                P(None, ("row", "dp")),
                P(("row", "dp"), None),
            ),
            check_vma=False,
        )

    return run
```
